512 devices in a mesh: grp: 128 (over y, x_lo, z), blk: 4 (over x_hi, core).
Axes of the slice: x: 4 (x_hi: 2, x_lo: 2; x = x_hi * 2 + x_lo), y: 8, z: 8, core: 2. Of those that a mesh axis runs over, the one named last changes fastest.
Arguments:
- amplitudes: bfloat16 [2048, 128, 512], P('grp', 'blk'), may hold values from -6 to 6
- integrals: float32 [2048, 12, 128, 128], P(('grp', 'blk')), may hold values from -0.15625 to 0.15625
- tile_rows: int32 [2048, 12], P(('grp', 'blk')), may hold values from 0 to 2047, as said below
- destinations: int32 [2048, 4], replicated, may hold values from 0 to 127, as said below
- source_terms: bfloat16 [262144, 512], P(('grp', 'blk')), may hold values from -6 to 6
- occ_energy: float32 [512], replicated, may hold values from 0.5 to 4
- virt_energy: float32 [262144], P(('grp', 'blk')), may hold values from 0.5 to 4
Outputs:
- new_amplitudes: bfloat16 [262144, 512], P(('grp', 'blk'))
The draws below stay inside these ranges and needn't reach their ends.
Inputs may be any that keep to these rules, and one draw needn't show every extreme that they name: `destinations`: each row names 4 different groups. Every group is named by exactly 64 rows in all. Among the 16 rows k of one owning group k // 16, no group is named by more than 2 rows, and that many is reached. `tile_rows`: the 12 entries of a row are different.
All inputs are finite; a program needn't handle non-finite values.
Results may differ from the reference program's by a relative error of at most 0.001.
Values may be sent and summed in bfloat16 or wider, within the bound.
No kernel may reach another device: no remote copies, remote signals or barrier semaphores. Data moves between devices by JAX's collectives and lax.ppermute only.
A program may use at most 64 MiB of HBM per device.

```python
import math
import jax
import jax.numpy as jnp
from jax import lax

TILE = 128
P_SIZE = 512
TILES_GRP = 16
DEST = 4
RT = 12
KT = 2048
USED = 32
RECV = 64
N_GRP = 128


def make_destinations(key):
    folded = jax.random.fold_in(key, 11)
    key_offsets, key_rows, key_mixing = jax.random.split(folded, 3)
    scores = jax.random.permutation(key_offsets, N_GRP).astype(jnp.int32)
    values = jnp.arange(N_GRP, dtype=jnp.int32)
    scores = jnp.where(values == 1, -2, scores)
    scores = jnp.where(values == N_GRP // 2, -1, scores)
    ranked = jnp.argsort(scores).astype(jnp.int32)
    leading = ranked[:USED]
    offsets = leading[jax.random.permutation(key_mixing, USED)]
    pattern = jnp.arange(TILES_GRP * DEST, dtype=jnp.int32).reshape(TILES_GRP, DEST) % USED
    offset_table = offsets[pattern]
    row_orders = jax.vmap(lambda subkey: jax.random.permutation(subkey, TILES_GRP))(jax.random.split(key_rows, N_GRP))
    owner_ids = jnp.arange(N_GRP, dtype=jnp.int32)[:, None, None]
    result = (owner_ids + offset_table[row_orders]) % N_GRP
    return result.reshape(KT, DEST).astype(jnp.int32)


def draw_destinations(key, part):
    return make_destinations(key)


def draw_tile_rows(key, part):
    targets = make_destinations(key)
    group_ids = jnp.arange(N_GRP, dtype=jnp.int32)
    member = jnp.any(targets[None, :, :] == group_ids[:, None, None], axis=2)
    tile_ids = jnp.arange(KT, dtype=jnp.int32)
    order_key = jnp.where(member, tile_ids[None, :], tile_ids[None, :] + KT)
    ordering = jnp.argsort(order_key, axis=1).astype(jnp.int32)
    folded = jax.random.fold_in(key, 23)
    key_one, key_two, key_three, key_four = jax.random.split(folded, 4)
    live_count = RT - 2
    col_local = jnp.arange(TILES_GRP, dtype=jnp.int32)[:, None] * live_count + jnp.arange(live_count, dtype=jnp.int32)[None, :]
    shuffles = jax.vmap(lambda subkey: jax.random.permutation(subkey, RECV))(jax.random.split(key_one, N_GRP))
    positions = shuffles[:, col_local % RECV]
    chosen = jax.vmap(lambda order_row, pick_row: order_row[pick_row])(ordering, positions)
    rest_count = KT - RECV
    first_pick = jax.random.randint(key_two, (N_GRP, TILES_GRP), 0, rest_count)
    gap_size = jax.random.randint(key_three, (N_GRP, TILES_GRP), 1, rest_count)
    second = (first_pick + gap_size) % rest_count
    extra_pos = RECV + jnp.stack([first_pick, second], axis=-1)
    extra_rows = jax.vmap(lambda order_row, pick_row: order_row[pick_row])(ordering, extra_pos)
    all_rows = jnp.concatenate([chosen, extra_rows], axis=-1).reshape(KT, RT)
    within = jax.vmap(lambda subkey: jax.random.permutation(subkey, RT))(jax.random.split(key_four, KT))
    return jnp.take_along_axis(all_rows, within, axis=1).astype(jnp.int32)


def level_of(stream_key, extent, shards, low, high):
    factor_of, own = 1.0, jax.random.fold_in(stream_key, 6)
    for axis_at, parts in shards:
        draws = jnp.exp(jax.random.uniform(jax.random.fold_in(own, axis_at), (parts,), jnp.float32, low / len(shards), high / len(shards)))
        factor_of = factor_of * jnp.repeat(draws, extent[axis_at] // parts).reshape([-1 if axis == axis_at else 1 for axis in range(len(extent))])
    return factor_of


def gaussian(key, dims, scale, most, cuts=(), held_as=jnp.bfloat16):
    entries = jax.random.normal(key, dims, jnp.float32) * scale
    if len(cuts) > 0:
        entries = level_of(key, dims, cuts, -0.22, 0.18) * entries
    return jnp.clip(entries, min=-most, max=most).astype(held_as)


def setup_inputs(seed: int = 0) -> dict:
    key_of = jax.random.split(jax.random.key(seed), 8)
    amplitudes = gaussian(key_of[0], (KT, TILE, P_SIZE), 1.0, 6.0, ((0, 128), (1, 4)))
    integrals = gaussian(key_of[1], (KT, RT, TILE, TILE), (RT * TILE) ** -0.5, 0.15625, ((0, 512),), jnp.float32)
    tile_rows = draw_tile_rows(jax.random.fold_in(key_of[7], 71), 0)
    destinations = draw_destinations(jax.random.fold_in(key_of[7], 71), 0)
    source_terms = gaussian(key_of[4], (KT * TILE, P_SIZE), 1.0, 6.0, ((0, 512),))
    occ_energy = jnp.clip(jnp.exp(jax.random.uniform(key_of[5], (P_SIZE,), jnp.float32, math.log(0.5), math.log(4.0))), 0.5, 4.0)
    virt_energy = jnp.clip(jnp.exp(math.log(4.0) - 2.0794415 * jax.random.uniform(key_of[6], (KT * TILE,), jnp.float32) ** level_of(key_of[6], (KT * TILE,), ((0, 512),), -0.2, 0.2)), 0.5, 4.0)
    return dict(amplitudes=amplitudes, integrals=integrals, tile_rows=tile_rows, destinations=destinations, source_terms=source_terms, occ_energy=occ_energy, virt_energy=virt_energy)


def reference(amplitudes, integrals, tile_rows, destinations, source_terms, occ_energy, virt_energy):
    owners = jnp.arange(KT, dtype=jnp.int32) // TILES_GRP
    named = jnp.any(destinations[tile_rows] == owners[:, None, None], axis=2)
    weight = named.astype(jnp.float32)

    def one_column(operands):
        tiles, rows_here, mask_here = operands
        picked = amplitudes[rows_here].astype(jnp.float32)
        scaled = tiles * mask_here[:, None, None]
        return jnp.einsum("rck,rcp->kp", scaled, picked, precision=lax.Precision.HIGHEST)

    ladder = lax.map(one_column, (integrals, tile_rows, weight))
    ladder = ladder.reshape(KT * TILE, P_SIZE)
    denominator = virt_energy[:, None] + occ_energy[None, :]
    return ((source_terms.astype(jnp.float32) + ladder) / denominator).astype(jnp.bfloat16)
```

```python
import jax
import jax.numpy as jnp
from jax import lax
from jax.experimental import pallas as pl
from jax.experimental.pallas import tpu as pltpu
from jax.sharding import Mesh, PartitionSpec as P

GRP = ("y", "xl", "z")
BLK = ("xh", "k")
SPREAD_A = ("y", "xh", "k")
SPREAD_B = ("xl", "z")
BF = jnp.bfloat16
F32 = jnp.float32


def route_kernel(groups, slots, tiles, width):
    step = 8
    lanes = 128

    def body(own_ref, dest_ref, table_ref, out_ref, mine_ref, slot_ref):
        ids = lax.broadcasted_iota(jnp.int32, (groups, lanes), 0)
        before = lax.broadcasted_iota(jnp.int32, (lanes, lanes), 0)
        after = lax.broadcasted_iota(jnp.int32, (lanes, lanes), 1)
        tri = (before < after).astype(F32).astype(BF)
        carry = jnp.zeros((groups, 1), F32)
        for i in range(tiles // lanes):
            named = dest_ref[0:1, pl.ds(i * lanes, lanes)] == ids
            for l in range(1, dest_ref.shape[0]):
                named = named | (dest_ref[l : l + 1, pl.ds(i * lanes, lanes)] == ids)
            ones = named.astype(F32)
            earlier = jnp.dot(ones.astype(BF), tri, preferred_element_type=F32) + carry
            slot_ref[:, pl.ds(i * lanes, lanes)] = jnp.where(named, earlier, -1.0)
            carry = carry + jnp.sum(ones, axis=1, keepdims=True)
        mine_ref[...] = slot_ref[pl.ds(own_ref[0], 1), :].astype(jnp.int32)
        place = lax.broadcasted_iota(jnp.int32, (1, slots, tiles), 1).astype(F32)

        def some_groups(g, _):
            rows = slot_ref[pl.ds(g * step, step), :]
            pick = (rows[:, None, :] == place).astype(F32).astype(BF)
            pick = pick.reshape(step * slots, tiles)
            got = jnp.dot(pick, table_ref[...], preferred_element_type=F32)
            out_ref[pl.ds(g * step * slots, step * slots), :] = got.astype(BF)
            return 0

        lax.fori_loop(0, groups // step, some_groups, 0)

    def call(own, dest, table):
        return pl.pallas_call(
            body,
            grid_spec=pltpu.PrefetchScalarGridSpec(
                num_scalar_prefetch=1,
                grid=(1,),
                in_specs=[
                    pl.BlockSpec(dest.shape, lambda i, s: (0, 0)),
                    pl.BlockSpec(table.shape, lambda i, s: (0, 0)),
                ],
                out_specs=[
                    pl.BlockSpec((groups * slots, width), lambda i, s: (0, 0)),
                    pl.BlockSpec((1, tiles), lambda i, s: (0, 0)),
                ],
                scratch_shapes=[pltpu.VMEM((groups, tiles), F32)],
            ),
            out_shape=[
                jax.ShapeDtypeStruct((groups * slots, width), BF),
                jax.ShapeDtypeStruct((1, tiles), jnp.int32),
            ],
            compiler_params=pltpu.CompilerParams(vmem_limit_bytes=48 * 1024 * 1024),
            name="route",
        )(own, dest, table)

    return call


def ladder_call(slot, weights, tiles):
    columns, listed, depth, size = weights.shape
    held, _, width = tiles.shape

    def body(slot_ref, w_ref, t_ref, out_ref):
        n = pl.program_id(0)
        his, los, ts = [], [], []
        for r in range(listed):
            s = slot_ref[n * listed + r]
            w = jnp.where(s >= 0, w_ref[0, r], 0.0)
            hi = w.astype(BF)
            his.append(hi)
            los.append((w - hi.astype(F32)).astype(BF))
            ts.append(t_ref[jnp.maximum(s, 0)])
        hi = jnp.concatenate(his, axis=0)
        lo = jnp.concatenate(los, axis=0)
        t = jnp.concatenate(ts, axis=0)
        both = jnp.concatenate([hi, lo], axis=1)
        acc = lax.dot_general(both, t, (((0,), (0,)), ((), ())), preferred_element_type=F32)
        out_ref[0] = acc[:size] + acc[size:]

    return pl.pallas_call(
        body,
        grid_spec=pltpu.PrefetchScalarGridSpec(
            num_scalar_prefetch=1,
            grid=(columns,),
            in_specs=[
                pl.BlockSpec((1, listed, depth, size), lambda n, s: (n, 0, 0, 0)),
                pl.BlockSpec((held, depth, width), lambda n, s: (0, 0, 0)),
            ],
            out_specs=pl.BlockSpec((1, size, width), lambda n, s: (n, 0, 0)),
        ),
        out_shape=jax.ShapeDtypeStruct((columns, size, width), F32),
        compiler_params=pltpu.CompilerParams(vmem_limit_bytes=48 * 1024 * 1024),
        name="ladder",
    )(slot, weights, tiles)


def per_device(amplitudes, integrals, tile_rows, destinations, source_terms, occ_energy, virt_energy):
    ny, nx, nz = (lax.axis_size(a) for a in GRP)
    nblk = lax.axis_size("xh") * lax.axis_size("k")
    groups = ny * nx * nz
    own = lax.axis_index(GRP).astype(jnp.int32)
    owned, rows, full_width = amplitudes.shape
    all_tiles, dest = destinations.shape
    width = full_width // nblk
    nc = nx * nz
    sub = rows // ny
    depth = rows * nblk
    slots = all_tiles * dest // groups
    columns, listed, _, size = integrals.shape

    weights = lax.all_gather(integrals, BLK, axis=0, tiled=True)
    named_tiles = lax.all_gather(tile_rows, BLK, axis=0, tiled=True)

    x = amplitudes.reshape(owned, ny, sub, nblk, width).transpose(1, 3, 2, 0, 4)
    x = x.reshape(ny * nblk, sub, owned, width)
    x = lax.all_to_all(x, SPREAD_A, 0, 0, tiled=True)
    x = x.reshape(ny, nblk * sub, owned, width).transpose(1, 0, 2, 3)
    x = lax.all_to_all(x, SPREAD_B, 0, 0, tiled=True)
    table = x.reshape(nc * ny * owned, width)

    dest_t = destinations.reshape(ny, nc, owned, dest).transpose(3, 1, 0, 2).reshape(dest, all_tiles)
    outgoing, mine = route_kernel(groups, slots, all_tiles, width)(own.reshape(1), dest_t, table)
    incoming = lax.all_to_all(outgoing.reshape(groups, slots, width), GRP, 0, 0, tiled=True)

    tiles = incoming.reshape(ny, nblk, sub, slots, width).transpose(3, 1, 0, 2, 4)
    tiles = tiles.reshape(slots, depth, width)

    y_of = named_tiles // (nc * owned)
    c_of = (named_tiles // owned) % nc
    at = c_of * (ny * owned) + y_of * owned + named_tiles % owned
    where = jnp.arange(all_tiles, dtype=jnp.int32)
    slot = jnp.max(jnp.where(at[:, :, None] == where, mine.reshape(1, 1, all_tiles), -1), axis=2)

    ladder = ladder_call(slot.reshape(-1), weights, tiles)
    ladder = ladder.reshape(nblk, columns * size, width)
    ladder = lax.all_to_all(ladder, BLK, 0, 0, tiled=True)
    ladder = ladder.transpose(1, 0, 2).reshape(columns * size, full_width)
    denominator = virt_energy[:, None] + occ_energy[None, :]
    return ((source_terms.astype(F32) + ladder) / denominator).astype(BF)


def solution(mesh):
    n_grp = mesh.shape["grp"]
    fine = Mesh(mesh.devices.reshape(8, 2, n_grp // 16, 2, 2), GRP + BLK)
    ALL = GRP + BLK
    in_specs = (
        P(GRP, BLK, None),
        P(ALL, None, None, None),
        P(ALL, None),
        P(),
        P(ALL, None),
        P(),
        P(ALL),
    )
    return jax.shard_map(
        per_device, mesh=fine, in_specs=in_specs, out_specs=P(ALL, None), check_vma=False
    )
```

```python
import jax
import jax.numpy as jnp
from jax import lax
from jax.experimental import pallas as pl
from jax.experimental.pallas import tpu as pltpu
from jax.sharding import Mesh, PartitionSpec as P

GRP = ("y", "xl", "z")
BLK = ("xh", "k")
LINE = ("xl", "xh", "k")
PLANE = ("y", "z")
BF = jnp.bfloat16
F32 = jnp.float32
PARAMS = pltpu.CompilerParams(vmem_limit_bytes=48 * 1024 * 1024)


def rank_call(own, dest, groups):
    named_by, tiles = dest.shape
    lanes = 128
    half = tiles // 2 // lanes

    def body(own_ref, dest_ref, slot_ref, early_ref, mine_ref):
        ids = lax.broadcasted_iota(jnp.int32, (groups, lanes), 0)
        before = lax.broadcasted_iota(jnp.int32, (lanes, lanes), 0)
        after = lax.broadcasted_iota(jnp.int32, (lanes, lanes), 1)
        tri = (before < after).astype(F32).astype(BF)
        carry = jnp.zeros((groups, 1), F32)
        for i in range(tiles // lanes):
            if i == half:
                early_ref[...] = jnp.broadcast_to(carry, (groups, lanes))
            named = dest_ref[0:1, pl.ds(i * lanes, lanes)] == ids
            for l in range(1, named_by):
                named = named | (dest_ref[l : l + 1, pl.ds(i * lanes, lanes)] == ids)
            ones = named.astype(F32)
            earlier = jnp.dot(ones.astype(BF), tri, preferred_element_type=F32) + carry
            slot_ref[:, pl.ds(i * lanes, lanes)] = jnp.where(named, earlier, -1.0)
            carry = carry + jnp.sum(ones, axis=1, keepdims=True)
        mine_ref[...] = slot_ref[pl.ds(own_ref[0], 1), :].astype(jnp.int32)

    return pl.pallas_call(
        body,
        grid_spec=pltpu.PrefetchScalarGridSpec(
            num_scalar_prefetch=1,
            grid=(1,),
            in_specs=[pl.BlockSpec(dest.shape, lambda i, s: (0, 0))],
            out_specs=[
                pl.BlockSpec((groups, tiles), lambda i, s: (0, 0)),
                pl.BlockSpec((groups, lanes), lambda i, s: (0, 0)),
                pl.BlockSpec((1, tiles), lambda i, s: (0, 0)),
            ],
        ),
        out_shape=[
            jax.ShapeDtypeStruct((groups, tiles), F32),
            jax.ShapeDtypeStruct((groups, lanes), F32),
            jax.ShapeDtypeStruct((1, tiles), jnp.int32),
        ],
        compiler_params=PARAMS,
        name="rank",
    )(own, dest)


def route_call(slot, early, table, slots):
    groups, tiles = slot.shape
    width = table.shape[1]
    half = tiles // 2
    step = 32
    deep = 16

    def body(slot_ref, early_ref, table_ref, out_ref):
        one = jnp.asarray(1, BF)
        zero = jnp.asarray(0, BF)
        place = lax.broadcasted_iota(jnp.int32, (deep, half), 0)
        places = [(place + deep * q).astype(F32).astype(BF) for q in range(slots // deep)]
        rows = slot_ref[...]
        parts = []
        for d in range(step):
            lo = jnp.broadcast_to(rows[d : d + 1, :half], (deep, half)).astype(BF)
            hi = jnp.broadcast_to(rows[d : d + 1, half:], (deep, half)).astype(BF)
            for at in places:
                parts.append(jnp.where((lo == at) | (hi == at), one, zero))
        pick = jnp.concatenate(parts, axis=0)
        both = jnp.concatenate([table_ref[:half, :], table_ref[half:, :]], axis=1)
        got = jnp.dot(pick, both, preferred_element_type=F32)
        j = lax.broadcasted_iota(jnp.int32, (slots, width), 0).astype(F32)
        for d in range(step):
            late = j >= early_ref[d : d + 1, :]
            g = got[d * slots : (d + 1) * slots]
            out_ref[d * slots : (d + 1) * slots, :] = jnp.where(late, g[:, width:], g[:, :width]).astype(BF)

    return pl.pallas_call(
        body,
        grid=(groups // step,),
        in_specs=[
            pl.BlockSpec((step, tiles), lambda i: (i, 0)),
            pl.BlockSpec((step, width), lambda i: (i, 0)),
            pl.BlockSpec((tiles, width), lambda i: (0, 0)),
        ],
        out_specs=pl.BlockSpec((step * slots, width), lambda i: (i, 0)),
        out_shape=jax.ShapeDtypeStruct((groups * slots, width), BF),
        compiler_params=PARAMS,
        name="route",
    )(slot, early, table)


def turn_call(tiles):
    slots, depth, width = tiles.shape
    step = 8

    def body(t_ref, out_ref):
        for i in range(step):
            out_ref[i] = t_ref[i].T

    return pl.pallas_call(
        body,
        grid=(slots // step,),
        in_specs=[pl.BlockSpec((step, depth, width), lambda i: (i, 0, 0))],
        out_specs=pl.BlockSpec((step, width, depth), lambda i: (i, 0, 0)),
        out_shape=jax.ShapeDtypeStruct((slots, width, depth), BF),
        compiler_params=PARAMS,
        name="turn",
    )(tiles)


def ladder_call(slot, base, weights, turned):
    columns, listed, depth, size = weights.shape
    width = turned.shape[1]

    def body(slot_ref, base_ref, w_ref, t_ref, out_ref):
        for n in range(columns):
            right, left = [], []
            for r in range(listed):
                s = slot_ref[base_ref[0] + n * listed + r]
                w = w_ref[n, r]
                hi = w.astype(BF)
                lo = (w - hi.astype(F32)).astype(BF)
                right.append(jnp.concatenate([hi, lo], axis=1))
                t = t_ref[jnp.maximum(s, 0)]
                left.append(jnp.where(s >= 0, t, jnp.zeros_like(t)))
            right = jnp.concatenate(right, axis=0)
            left = jnp.concatenate(left, axis=1)
            acc = jnp.dot(left, right, preferred_element_type=F32)
            out_ref[n * size : (n + 1) * size, :] = (acc[:, :size] + acc[:, size:]).T

    return pl.pallas_call(
        body,
        grid_spec=pltpu.PrefetchScalarGridSpec(
            num_scalar_prefetch=2,
            grid=(1,),
            in_specs=[
                pl.BlockSpec(weights.shape, lambda i, s, b: (0, 0, 0, 0)),
                pl.BlockSpec(turned.shape, lambda i, s, b: (0, 0, 0)),
            ],
            out_specs=pl.BlockSpec((columns * size, width), lambda i, s, b: (0, 0)),
        ),
        out_shape=jax.ShapeDtypeStruct((columns * size, width), F32),
        compiler_params=PARAMS,
        name="ladder",
    )(slot, base, weights, turned)


def finish_call(blk, pieces, source, occ, virt):
    rows, width = pieces[0].shape
    count = len(pieces)
    tall, size = virt.shape

    def body(blk_ref, *refs):
        piece_refs = refs[:count]
        s_ref, o_ref, v_ref, out_ref = refs[count:]
        i = pl.program_id(0)
        for j in range(count):

            @pl.when(i == j)
            def _(j=j):
                for n in range(tall):
                    at = slice(n * size, (n + 1) * size)
                    v = jnp.broadcast_to(v_ref[n : n + 1, :], (size, size)).T
                    total = s_ref[at, :].astype(F32) + piece_refs[j][at, :]
                    out_ref[at, :] = (total / (v + o_ref[...])).astype(BF)

    whole = pl.BlockSpec((rows, width), lambda i, b: (0, 0))
    part = pl.BlockSpec((rows, width), lambda i, b: (0, b[0] ^ i))
    return pl.pallas_call(
        body,
        grid_spec=pltpu.PrefetchScalarGridSpec(
            num_scalar_prefetch=1,
            grid=(count,),
            in_specs=[whole] * count
            + [part, pl.BlockSpec((1, width), lambda i, b: (0, b[0] ^ i)), pl.BlockSpec(virt.shape, lambda i, b: (0, 0))],
            out_specs=part,
        ),
        out_shape=jax.ShapeDtypeStruct(source.shape, BF),
        compiler_params=PARAMS,
        name="finish",
    )(blk, *pieces, source, occ, virt)


def swap(x, flip, n):
    return lax.ppermute(x, BLK, [(b, b ^ flip) for b in range(n)])


def per_device(amplitudes, integrals, tile_rows, destinations, source_terms, occ_energy, virt_energy):
    ny, nx, nz = (lax.axis_size(a) for a in GRP)
    nblk = lax.axis_size("xh") * lax.axis_size("k")
    groups = ny * nx * nz
    own = lax.axis_index(GRP).astype(jnp.int32)
    blk = lax.axis_index(BLK).astype(jnp.int32)
    owned, rows, full_width = amplitudes.shape
    all_tiles, dest = destinations.shape
    width = full_width // nblk
    sub = rows // nx
    slots = all_tiles * dest // groups
    columns, listed, _, size = integrals.shape

    x = amplitudes.reshape(owned, nx, sub, nblk, width).transpose(1, 3, 2, 0, 4)
    x = lax.all_to_all(x.reshape(nx * nblk, sub, owned, width), LINE, 0, 0, tiled=True)
    held, x = lax.optimization_barrier((integrals, x))
    across = swap(held, 2, nblk)
    x = x.reshape(nx, nblk, sub, owned, width).transpose(1, 2, 0, 3, 4)
    x = lax.all_to_all(x.reshape(ny * nz, nx * owned, width), PLANE, 0, 0, tiled=True)
    table = x.reshape(all_tiles, width)

    dest_t = destinations.reshape(ny, nx, nz, owned, dest).transpose(4, 0, 2, 1, 3)
    slot_of, early, mine = rank_call(own.reshape(1), dest_t.reshape(dest, all_tiles), groups)
    outgoing = route_call(slot_of, early, table, slots)
    incoming = lax.all_to_all(outgoing.reshape(groups, slots, width), GRP, 0, 0, tiled=True)

    beside = swap(held, 1, nblk)
    named_tiles = lax.all_gather(tile_rows, BLK, axis=0, tiled=True)
    y_of = named_tiles // (nx * nz * owned)
    x_of = (named_tiles // (nz * owned)) % nx
    z_of = (named_tiles // owned) % nz
    at = ((y_of * nz + z_of) * nx + x_of) * owned + named_tiles % owned
    where = jnp.arange(all_tiles, dtype=jnp.int32)
    slot = jnp.max(jnp.where(at[:, :, None] == where, mine.reshape(1, 1, all_tiles), -1), axis=2)
    slot = slot.reshape(-1)
    diagonal = swap(across, 1, nblk)

    tiles = incoming.reshape(nblk, ny // nblk, nx, nz, slots, width).transpose(4, 0, 2, 1, 3, 5)
    turned = turn_call(tiles.reshape(slots, rows * nblk, width))

    def partial(flip, weights):
        base = (blk ^ flip) * (columns * listed)
        return ladder_call(slot, base.reshape(1), weights, turned)

    far = swap(partial(2, across), 2, nblk)
    farther = swap(partial(3, diagonal), 3, nblk)
    near = swap(partial(1, beside), 1, nblk)
    home = partial(0, integrals)
    return finish_call(
        blk.reshape(1),
        (home, near, far, farther),
        source_terms,
        occ_energy.reshape(1, full_width),
        virt_energy.reshape(columns, size),
    )


def solution(mesh):
    n_grp = mesh.shape["grp"]
    fine = Mesh(mesh.devices.reshape(8, 2, n_grp // 16, 2, 2), GRP + BLK)
    every = GRP + BLK
    in_specs = (
        P(GRP, BLK, None),
        P(every, None, None, None),
        P(every, None),
        P(),
        P(every, None),
        P(),
        P(every),
    )
    return jax.shard_map(
        per_device, mesh=fine, in_specs=in_specs, out_specs=P(every, None), check_vma=False
    )
```

```python
import jax
import jax.numpy as jnp
from jax import lax
from jax.experimental import pallas as pl
from jax.experimental.pallas import tpu as pltpu
from jax.sharding import Mesh, PartitionSpec as P


GRP = ("y", "xl", "z")
BLK = ("xh", "k")
LINE = ("xl", "xh", "k")
PLANE = ("y", "z")
BF = jnp.bfloat16
F32 = jnp.float32
PARAMS = pltpu.CompilerParams(vmem_limit_bytes=48 * 1024 * 1024)


def rank_call(own, dest, groups):
    named_by, tiles = dest.shape
    lanes = 128
    half = tiles // 2 // lanes

    def body(own_ref, dest_ref, slot_ref, early_ref, mine_ref):
        ids = lax.broadcasted_iota(jnp.int32, (groups, lanes), 0)
        before = lax.broadcasted_iota(jnp.int32, (lanes, lanes), 0)
        after = lax.broadcasted_iota(jnp.int32, (lanes, lanes), 1)
        tri = (before < after).astype(F32).astype(BF)
        carry = jnp.zeros((groups, 1), F32)
        for i in range(tiles // lanes):
            if i == half:
                early_ref[...] = jnp.broadcast_to(carry, (groups, lanes))
            named = dest_ref[0:1, pl.ds(i * lanes, lanes)] == ids
            for l in range(1, named_by):
                named = named | (dest_ref[l : l + 1, pl.ds(i * lanes, lanes)] == ids)
            ones = named.astype(F32)
            earlier = jnp.dot(ones.astype(BF), tri, preferred_element_type=F32) + carry
            slot_ref[:, pl.ds(i * lanes, lanes)] = jnp.where(named, earlier, -1.0)
            carry = carry + jnp.sum(ones, axis=1, keepdims=True)
        mine_ref[...] = slot_ref[pl.ds(own_ref[0], 1), :].astype(jnp.int32)

    return pl.pallas_call(
        body,
        grid_spec=pltpu.PrefetchScalarGridSpec(
            num_scalar_prefetch=1,
            grid=(1,),
            in_specs=[pl.BlockSpec(dest.shape, lambda i, s: (0, 0))],
            out_specs=[
                pl.BlockSpec((groups, tiles), lambda i, s: (0, 0)),
                pl.BlockSpec((groups, lanes), lambda i, s: (0, 0)),
                pl.BlockSpec((1, tiles), lambda i, s: (0, 0)),
            ],
        ),
        out_shape=[
            jax.ShapeDtypeStruct((groups, tiles), F32),
            jax.ShapeDtypeStruct((groups, lanes), F32),
            jax.ShapeDtypeStruct((1, tiles), jnp.int32),
        ],
        compiler_params=PARAMS,
        name="rank",
    )(own, dest)


def route_call(slot, early, table, slots):
    groups, tiles = slot.shape
    width = table.shape[1]
    half = tiles // 2
    step = 32
    deep = 16

    def body(slot_ref, early_ref, table_ref, out_ref):
        one = jnp.asarray(1, BF)
        zero = jnp.asarray(0, BF)
        place = lax.broadcasted_iota(jnp.int32, (deep, half), 0)
        places = [(place + deep * q).astype(F32).astype(BF) for q in range(slots // deep)]
        rows = slot_ref[...]
        parts = []
        for d in range(step):
            lo = jnp.broadcast_to(rows[d : d + 1, :half], (deep, half)).astype(BF)
            hi = jnp.broadcast_to(rows[d : d + 1, half:], (deep, half)).astype(BF)
            for at in places:
                parts.append(jnp.where((lo == at) | (hi == at), one, zero))
        pick = jnp.concatenate(parts, axis=0)
        both = jnp.concatenate([table_ref[:half, :], table_ref[half:, :]], axis=1)
        got = jnp.dot(pick, both, preferred_element_type=F32)
        j = lax.broadcasted_iota(jnp.int32, (slots, width), 0).astype(F32)
        for d in range(step):
            late = j >= early_ref[d : d + 1, :]
            g = got[d * slots : (d + 1) * slots]
            out_ref[d * slots : (d + 1) * slots, :] = jnp.where(late, g[:, width:], g[:, :width]).astype(BF)

    return pl.pallas_call(
        body,
        grid=(groups // step,),
        in_specs=[
            pl.BlockSpec((step, tiles), lambda i: (i, 0)),
            pl.BlockSpec((step, width), lambda i: (i, 0)),
            pl.BlockSpec((tiles, width), lambda i: (0, 0)),
        ],
        out_specs=pl.BlockSpec((step * slots, width), lambda i: (i, 0)),
        out_shape=jax.ShapeDtypeStruct((groups * slots, width), BF),
        compiler_params=PARAMS,
        name="route",
    )(slot, early, table)


def turn_call(tiles):
    slots, depth, width = tiles.shape
    step = 8

    def body(t_ref, out_ref):
        for i in range(step):
            out_ref[i] = t_ref[i].T

    return pl.pallas_call(
        body,
        grid=(slots // step,),
        in_specs=[pl.BlockSpec((step, depth, width), lambda i: (i, 0, 0))],
        out_specs=pl.BlockSpec((step, width, depth), lambda i: (i, 0, 0)),
        out_shape=jax.ShapeDtypeStruct((slots, width, depth), BF),
        compiler_params=PARAMS,
        name="turn",
    )(tiles)


def ladder_call(slot, base, weights, turned):
    columns, listed, depth, size = weights.shape
    width = turned.shape[1]
    some = columns // 2

    def body(slot_ref, w_ref, t_ref, out_ref):
        first = pl.program_id(0) * some
        for n in range(some):
            right, left = [], []
            for r in range(listed):
                s = slot_ref[base + (first + n) * listed + r]
                w = w_ref[n, r]
                hi = w.astype(BF)
                lo = (w - hi.astype(F32)).astype(BF)
                right.append(jnp.concatenate([hi, lo], axis=1))
                t = t_ref[jnp.maximum(s, 0)]
                left.append(jnp.where(s >= 0, t, jnp.zeros_like(t)))
            right = jnp.concatenate(right, axis=0)
            left = jnp.concatenate(left, axis=1)
            acc = jnp.dot(left, right, preferred_element_type=F32)
            out_ref[n * size : (n + 1) * size, :] = (acc[:, :size] + acc[:, size:]).T

    return pl.pallas_call(
        body,
        grid_spec=pltpu.PrefetchScalarGridSpec(
            num_scalar_prefetch=1,
            grid=(2,),
            in_specs=[
                pl.BlockSpec((some, listed, depth, size), lambda i, s: (i, 0, 0, 0)),
                pl.BlockSpec(turned.shape, lambda i, s: (0, 0, 0)),
            ],
            out_specs=pl.BlockSpec((some * size, width), lambda i, s: (i, 0)),
        ),
        out_shape=jax.ShapeDtypeStruct((columns * size, width), F32),
        compiler_params=PARAMS,
        name="ladder",
    )(slot, weights, turned)


def finish_call(blk, pieces, source, occ, virt):
    rows, width = pieces[0].shape
    count = len(pieces)
    tall, size = virt.shape

    def body(blk_ref, *refs):
        piece_refs = refs[:count]
        s_ref, o_ref, v_ref, out_ref = refs[count:]
        i = pl.program_id(0)
        for j in range(count):

            @pl.when(i == j)
            def _(j=j):
                for n in range(tall):
                    at = slice(n * size, (n + 1) * size)
                    v = jnp.broadcast_to(v_ref[n : n + 1, :], (size, size)).T
                    total = s_ref[at, :].astype(F32) + piece_refs[j][at, :]
                    out_ref[at, :] = (total / (v + o_ref[...])).astype(BF)

    whole = pl.BlockSpec((rows, width), lambda i, b: (0, 0))
    part = pl.BlockSpec((rows, width), lambda i, b: (0, b[0] ^ i))
    return pl.pallas_call(
        body,
        grid_spec=pltpu.PrefetchScalarGridSpec(
            num_scalar_prefetch=1,
            grid=(count,),
            in_specs=[whole] * count
            + [part, pl.BlockSpec((1, width), lambda i, b: (0, b[0] ^ i)), pl.BlockSpec(virt.shape, lambda i, b: (0, 0))],
            out_specs=part,
        ),
        out_shape=jax.ShapeDtypeStruct(source.shape, BF),
        compiler_params=PARAMS,
        name="finish",
    )(blk, *pieces, source, occ, virt)


def swap(x, flip, n):
    return lax.ppermute(x, BLK, [(b, b ^ flip) for b in range(n)])


def per_device(amplitudes, integrals, tile_rows, destinations, source_terms, occ_energy, virt_energy):
    ny, nx, nz = (lax.axis_size(a) for a in GRP)
    nblk = lax.axis_size("xh") * lax.axis_size("k")
    groups = ny * nx * nz
    own = lax.axis_index(GRP).astype(jnp.int32)
    blk = lax.axis_index(BLK).astype(jnp.int32)
    owned, rows, full_width = amplitudes.shape
    all_tiles, dest = destinations.shape
    width = full_width // nblk
    sub = rows // nx
    slots = all_tiles * dest // groups
    columns, listed, _, size = integrals.shape

    x = amplitudes.reshape(owned, nx, sub, nblk, width).transpose(1, 3, 2, 0, 4)
    x = lax.all_to_all(x.reshape(nx * nblk, sub, owned, width), LINE, 0, 0, tiled=True)
    rows_across = swap(tile_rows, 2, nblk)
    across = swap(integrals, 2, nblk)
    x = x.reshape(nx, nblk, sub, owned, width).transpose(1, 2, 0, 3, 4)
    x = lax.all_to_all(x.reshape(ny * nz, nx * owned, width), PLANE, 0, 0, tiled=True)
    table = x.reshape(all_tiles, width)

    dest_t = destinations.reshape(ny, nx, nz, owned, dest).transpose(4, 0, 2, 1, 3)
    slot_of, early, mine = rank_call(own.reshape(1), dest_t.reshape(dest, all_tiles), groups)
    outgoing = route_call(slot_of, early, table, slots)
    incoming = lax.all_to_all(outgoing.reshape(groups, slots, width), GRP, 0, 0, tiled=True)

    beside = swap(integrals, 1, nblk)
    near_rows = jnp.concatenate([tile_rows, rows_across], axis=0)
    far_rows = swap(near_rows, 1, nblk)
    named_tiles = jnp.concatenate([near_rows, far_rows], axis=0)
    y_of = named_tiles // (nx * nz * owned)
    x_of = (named_tiles // (nz * owned)) % nx
    z_of = (named_tiles // owned) % nz
    at = ((y_of * nz + z_of) * nx + x_of) * owned + named_tiles % owned
    where = jnp.arange(all_tiles, dtype=jnp.int32)
    slot = jnp.max(jnp.where(at[:, :, None] == where, mine.reshape(1, 1, all_tiles), -1), axis=2)
    slot = slot.reshape(-1)
    diagonal = swap(across, 1, nblk)

    tiles = incoming.reshape(nblk, ny // nblk, nx, nz, slots, width).transpose(4, 0, 2, 1, 3, 5)
    turned = turn_call(tiles.reshape(slots, rows * nblk, width))

    def partial(place, weights):
        return ladder_call(slot, place * columns * listed, weights, turned)

    far = swap(partial(1, across), 2, nblk)
    farther = swap(partial(3, diagonal), 3, nblk)
    near = swap(partial(2, beside), 1, nblk)
    home = partial(0, integrals)
    return finish_call(
        blk.reshape(1),
        (home, near, far, farther),
        source_terms,
        occ_energy.reshape(1, full_width),
        virt_energy.reshape(columns, size),
    )


def solution(mesh):
    n_grp = mesh.shape["grp"]
    fine = Mesh(mesh.devices.reshape(8, 2, n_grp // 16, 2, 2), GRP + BLK)
    every = GRP + BLK
    in_specs = (
        P(GRP, BLK, None),
        P(every, None, None, None),
        P(every, None),
        P(),
        P(every, None),
        P(),
        P(every),
    )
    return jax.shard_map(
        per_device, mesh=fine, in_specs=in_specs, out_specs=P(every, None), check_vma=False
    )
```

```python
import jax
import jax.numpy as jnp
from jax import lax
from jax.experimental import pallas as pl
from jax.experimental.pallas import tpu as pltpu
from jax.sharding import Mesh, PartitionSpec as P


GRP = ("y", "xl", "z")
BLK = ("xh", "k")
LINE = ("xl", "xh", "k")
PLANE = ("y", "z")
BF = jnp.bfloat16
F32 = jnp.float32
PARAMS = pltpu.CompilerParams(vmem_limit_bytes=48 * 1024 * 1024)


def rank_call(own, dest, groups):
    named_by, tiles = dest.shape
    lanes = 128
    half = tiles // 2 // lanes

    def body(own_ref, dest_ref, slot_ref, early_ref, mine_ref):
        ids = lax.broadcasted_iota(jnp.int32, (groups, lanes), 0)
        before = lax.broadcasted_iota(jnp.int32, (lanes, lanes), 0)
        after = lax.broadcasted_iota(jnp.int32, (lanes, lanes), 1)
        tri = (before < after).astype(F32).astype(BF)
        carry = jnp.zeros((groups, 1), F32)
        for i in range(tiles // lanes):
            if i == half:
                early_ref[...] = jnp.broadcast_to(carry, (groups, lanes))
            named = dest_ref[0:1, pl.ds(i * lanes, lanes)] == ids
            for l in range(1, named_by):
                named = named | (dest_ref[l : l + 1, pl.ds(i * lanes, lanes)] == ids)
            ones = named.astype(F32)
            earlier = jnp.dot(ones.astype(BF), tri, preferred_element_type=F32) + carry
            slot_ref[:, pl.ds(i * lanes, lanes)] = jnp.where(named, earlier, -1.0)
            carry = carry + jnp.sum(ones, axis=1, keepdims=True)
        mine_ref[...] = slot_ref[pl.ds(own_ref[0], 1), :].astype(jnp.int32)

    return pl.pallas_call(
        body,
        grid_spec=pltpu.PrefetchScalarGridSpec(
            num_scalar_prefetch=1,
            grid=(1,),
            in_specs=[pl.BlockSpec(dest.shape, lambda i, s: (0, 0))],
            out_specs=[
                pl.BlockSpec((groups, tiles), lambda i, s: (0, 0)),
                pl.BlockSpec((groups, lanes), lambda i, s: (0, 0)),
                pl.BlockSpec((1, tiles), lambda i, s: (0, 0)),
            ],
        ),
        out_shape=[
            jax.ShapeDtypeStruct((groups, tiles), F32),
            jax.ShapeDtypeStruct((groups, lanes), F32),
            jax.ShapeDtypeStruct((1, tiles), jnp.int32),
        ],
        compiler_params=PARAMS,
        name="rank",
    )(own, dest)


def route_call(slot, early, table, slots):
    groups, tiles = slot.shape
    width = table.shape[1]
    half = tiles // 2
    step = 32
    deep = 16

    def body(slot_ref, early_ref, table_ref, out_ref):
        one = jnp.asarray(1, BF)
        zero = jnp.asarray(0, BF)
        place = lax.broadcasted_iota(jnp.int32, (deep, half), 0)
        places = [(place + deep * q).astype(F32).astype(BF) for q in range(slots // deep)]
        rows = slot_ref[...]
        parts = []
        for d in range(step):
            lo = jnp.broadcast_to(rows[d : d + 1, :half], (deep, half)).astype(BF)
            hi = jnp.broadcast_to(rows[d : d + 1, half:], (deep, half)).astype(BF)
            for at in places:
                parts.append(jnp.where((lo == at) | (hi == at), one, zero))
        pick = jnp.concatenate(parts, axis=0)
        both = jnp.concatenate([table_ref[:half, :], table_ref[half:, :]], axis=1)
        got = jnp.dot(pick, both, preferred_element_type=F32)
        j = lax.broadcasted_iota(jnp.int32, (slots, width), 0).astype(F32)
        for d in range(step):
            late = j >= early_ref[d : d + 1, :]
            g = got[d * slots : (d + 1) * slots]
            out_ref[d * slots : (d + 1) * slots, :] = jnp.where(late, g[:, width:], g[:, :width]).astype(BF)

    return pl.pallas_call(
        body,
        grid=(groups // step,),
        in_specs=[
            pl.BlockSpec((step, tiles), lambda i: (i, 0)),
            pl.BlockSpec((step, width), lambda i: (i, 0)),
            pl.BlockSpec((tiles, width), lambda i: (0, 0)),
        ],
        out_specs=pl.BlockSpec((step * slots, width), lambda i: (i, 0)),
        out_shape=jax.ShapeDtypeStruct((groups * slots, width), BF),
        compiler_params=PARAMS,
        name="route",
    )(slot, early, table)


def turn_call(tiles):
    slots, depth, width = tiles.shape
    step = 8

    def body(t_ref, out_ref):
        for i in range(step):
            out_ref[i] = t_ref[i].T

    return pl.pallas_call(
        body,
        grid=(slots // step,),
        in_specs=[pl.BlockSpec((step, depth, width), lambda i: (i, 0, 0))],
        out_specs=pl.BlockSpec((step, width, depth), lambda i: (i, 0, 0)),
        out_shape=jax.ShapeDtypeStruct((slots, width, depth), BF),
        compiler_params=PARAMS,
        name="turn",
    )(tiles)


def ladder_call(slot, blk, flips, weights, turned, sources, occ, virt):
    columns, listed, depth, size = weights[0].shape
    width = turned.shape[1]
    owners = len(weights)
    some = 2

    def body(slot_ref, blk_ref, *refs):
        w_refs = refs[:owners]
        t_ref = refs[owners]
        s_refs = refs[owners + 1 : 2 * owners + 1]
        o_ref, v_ref, out_ref, held_ref, sems = refs[2 * owners + 1 :]
        for m in range(owners):
            for n in range(columns):
                at = m * columns + n
                pltpu.make_async_copy(w_refs[m].at[n], held_ref.at[at], sems.at[at]).start()
        for m in range(owners):
            to = blk_ref[0] ^ flips[m]

            def some_columns(i, _, m=m, to=to):
                for u in range(some):
                    n = i * some + u
                    at = m * columns + n
                    pltpu.make_async_copy(w_refs[m].at[n], held_ref.at[at], sems.at[at]).wait()
                    right, left = [], []
                    for r in range(listed):
                        s = slot_ref[at * listed + r]
                        w = held_ref[at, r]
                        hi = w.astype(BF)
                        lo = (w - hi.astype(F32)).astype(BF)
                        right.append(jnp.concatenate([hi, lo], axis=1))
                        t = t_ref[jnp.maximum(s, 0)]
                        left.append(jnp.where(s >= 0, t, jnp.zeros_like(t)))
                    right = jnp.concatenate(right, axis=0)
                    left = jnp.concatenate(left, axis=1)
                    acc = jnp.dot(left, right, preferred_element_type=F32)
                    part = (acc[:, :size] + acc[:, size:]).T
                    rows = pl.ds(n * size, size)
                    total = s_refs[m][rows, :].astype(F32) + part
                    v = jnp.broadcast_to(v_ref[pl.ds(at, 1), :], (size, size)).T
                    out_ref[to, rows, :] = (total / (v + o_ref[...])).astype(BF)
                return 0

            lax.fori_loop(0, columns // some, some_columns, 0)

    def whole(x):
        return pl.BlockSpec(x.shape, lambda i, s, b: (0,) * x.ndim)

    return pl.pallas_call(
        body,
        grid_spec=pltpu.PrefetchScalarGridSpec(
            num_scalar_prefetch=2,
            grid=(1,),
            in_specs=[pl.BlockSpec(memory_space=pl.ANY)] * owners
            + [whole(turned)]
            + [whole(x) for x in sources]
            + [pl.BlockSpec((1, width), lambda i, s, b: (0, b[0])), whole(virt)],
            out_specs=pl.BlockSpec((owners, columns * size, width), lambda i, s, b: (0, 0, 0)),
            scratch_shapes=[
                pltpu.VMEM((owners * columns, listed, depth, size), F32),
                pltpu.SemaphoreType.DMA((owners * columns,)),
            ],
        ),
        out_shape=jax.ShapeDtypeStruct((owners, columns * size, width), BF),
        compiler_params=pltpu.CompilerParams(vmem_limit_bytes=48 * 1024 * 1024),
        name="ladder",
    )(slot, blk, *weights, turned, *sources, occ, virt)


def swap(x, flip, n):
    return lax.ppermute(x, BLK, [(b, b ^ flip) for b in range(n)])


def per_device(amplitudes, integrals, tile_rows, destinations, source_terms, occ_energy, virt_energy):
    ny, nx, nz = (lax.axis_size(a) for a in GRP)
    nblk = lax.axis_size("xh") * lax.axis_size("k")
    groups = ny * nx * nz
    own = lax.axis_index(GRP).astype(jnp.int32)
    blk = lax.axis_index(BLK).astype(jnp.int32)
    owned, rows, full_width = amplitudes.shape
    all_tiles, dest = destinations.shape
    width = full_width // nblk
    sub = rows // nx
    slots = all_tiles * dest // groups
    columns, listed, _, size = integrals.shape

    x = amplitudes.reshape(owned, nx, sub, nblk, width).transpose(1, 3, 2, 0, 4)
    x = lax.all_to_all(x.reshape(nx * nblk, sub, owned, width), LINE, 0, 0, tiled=True)
    facts = [virt_energy.reshape(columns, size), tile_rows.astype(F32)]
    facts.append(jnp.zeros((columns, size - listed), F32))
    facts = jnp.concatenate(facts, axis=1)
    facts_across = swap(facts, 2, nblk)
    across = swap(integrals, 2, nblk)
    x = x.reshape(nx, nblk, sub, owned, width).transpose(1, 2, 0, 3, 4)
    x = lax.all_to_all(x.reshape(ny * nz, nx * owned, width), PLANE, 0, 0, tiled=True)
    table = x.reshape(all_tiles, width)

    dest_t = destinations.reshape(ny, nx, nz, owned, dest).transpose(4, 0, 2, 1, 3)
    slot_of, early, mine = rank_call(own.reshape(1), dest_t.reshape(dest, all_tiles), groups)
    outgoing = route_call(slot_of, early, table, slots)
    incoming = lax.all_to_all(outgoing.reshape(groups, slots, width), GRP, 0, 0, tiled=True)

    beside = swap(integrals, 1, nblk)
    facts = jnp.concatenate([facts, facts_across], axis=0)
    facts = jnp.concatenate([facts, swap(facts, 1, nblk)], axis=0)
    named_tiles = facts[:, size : size + listed].astype(jnp.int32)
    y_of = named_tiles // (nx * nz * owned)
    x_of = (named_tiles // (nz * owned)) % nx
    z_of = (named_tiles // owned) % nz
    at = ((y_of * nz + z_of) * nx + x_of) * owned + named_tiles % owned
    where = jnp.arange(all_tiles, dtype=jnp.int32)
    slot = jnp.max(jnp.where(at[:, :, None] == where, mine.reshape(1, 1, all_tiles), -1), axis=2)
    slot = slot.reshape(-1)
    diagonal = swap(across, 1, nblk)

    tiles = incoming.reshape(nblk, ny // nblk, nx, nz, slots, width).transpose(4, 0, 2, 1, 3, 5)
    turned = turn_call(tiles.reshape(slots, rows * nblk, width))

    def quarter(flip):
        return lax.dynamic_slice_in_dim(source_terms, (blk ^ flip) * width, width, 1)

    source_far = swap(quarter(2), 2, nblk)
    source_near = swap(quarter(1), 1, nblk)
    source_diagonal = swap(quarter(3), 3, nblk)

    done = ladder_call(
        slot,
        blk.reshape(1),
        (0, 2, 1, 3),
        (integrals, across, beside, diagonal),
        turned,
        (quarter(0), source_far, source_near, source_diagonal),
        occ_energy.reshape(1, full_width),
        facts[:, :size],
    )
    done = lax.all_to_all(done, BLK, 0, 0, tiled=True)
    return done.transpose(1, 0, 2).reshape(columns * size, full_width)


def solution(mesh):
    n_grp = mesh.shape["grp"]
    fine = Mesh(mesh.devices.reshape(8, 2, n_grp // 16, 2, 2), GRP + BLK)
    every = GRP + BLK
    in_specs = (
        P(GRP, BLK, None),
        P(every, None, None, None),
        P(every, None),
        P(),
        P(every, None),
        P(),
        P(every),
    )
    return jax.shard_map(
        per_device, mesh=fine, in_specs=in_specs, out_specs=P(every, None), check_vma=False
    )
```

```python
import jax
import jax.numpy as jnp
from jax import lax
from jax.experimental import pallas as pl
from jax.experimental.pallas import tpu as pltpu
from jax.sharding import Mesh, PartitionSpec as P


GRP = ("y", "xl", "z")
BLK = ("xh", "k")
LINE = ("xl", "xh", "k")
PLANE = ("y", "z")
BF = jnp.bfloat16
F32 = jnp.float32
PARAMS = pltpu.CompilerParams(vmem_limit_bytes=48 * 1024 * 1024)


def rank_call(own, dest, groups):
    named_by, tiles = dest.shape
    lanes = 128
    half = tiles // 2 // lanes

    def body(own_ref, dest_ref, slot_ref, early_ref, mine_ref):
        ids = lax.broadcasted_iota(jnp.int32, (groups, lanes), 0)
        before = lax.broadcasted_iota(jnp.int32, (lanes, lanes), 0)
        after = lax.broadcasted_iota(jnp.int32, (lanes, lanes), 1)
        tri = (before < after).astype(F32).astype(BF)
        carry = jnp.zeros((groups, 1), F32)
        for i in range(tiles // lanes):
            if i == half:
                early_ref[...] = jnp.broadcast_to(carry, (groups, lanes))
            named = dest_ref[0:1, pl.ds(i * lanes, lanes)] == ids
            for l in range(1, named_by):
                named = named | (dest_ref[l : l + 1, pl.ds(i * lanes, lanes)] == ids)
            ones = named.astype(F32)
            earlier = jnp.dot(ones.astype(BF), tri, preferred_element_type=F32) + carry
            slot_ref[:, pl.ds(i * lanes, lanes)] = jnp.where(named, earlier, -1.0)
            carry = carry + jnp.sum(ones, axis=1, keepdims=True)
        mine_ref[...] = slot_ref[pl.ds(own_ref[0], 1), :].astype(jnp.int32)

    return pl.pallas_call(
        body,
        grid_spec=pltpu.PrefetchScalarGridSpec(
            num_scalar_prefetch=1,
            grid=(1,),
            in_specs=[pl.BlockSpec(dest.shape, lambda i, s: (0, 0))],
            out_specs=[
                pl.BlockSpec((groups, tiles), lambda i, s: (0, 0)),
                pl.BlockSpec((groups, lanes), lambda i, s: (0, 0)),
                pl.BlockSpec((1, tiles), lambda i, s: (0, 0)),
            ],
        ),
        out_shape=[
            jax.ShapeDtypeStruct((groups, tiles), F32),
            jax.ShapeDtypeStruct((groups, lanes), F32),
            jax.ShapeDtypeStruct((1, tiles), jnp.int32),
        ],
        compiler_params=PARAMS,
        name="rank",
    )(own, dest)


def route_call(slot, early, table, slots):
    groups, tiles = slot.shape
    width = table.shape[1]
    half = tiles // 2
    step = 32
    deep = 16

    def body(slot_ref, early_ref, table_ref, out_ref):
        one = jnp.asarray(1, BF)
        zero = jnp.asarray(0, BF)
        place = lax.broadcasted_iota(jnp.int32, (deep, half), 0)
        places = [(place + deep * q).astype(F32).astype(BF) for q in range(slots // deep)]
        rows = slot_ref[...]
        parts = []
        for d in range(step):
            lo = jnp.broadcast_to(rows[d : d + 1, :half], (deep, half)).astype(BF)
            hi = jnp.broadcast_to(rows[d : d + 1, half:], (deep, half)).astype(BF)
            for at in places:
                parts.append(jnp.where((lo == at) | (hi == at), one, zero))
        pick = jnp.concatenate(parts, axis=0)
        both = jnp.concatenate([table_ref[:half, :], table_ref[half:, :]], axis=1)
        got = jnp.dot(pick, both, preferred_element_type=F32)
        j = lax.broadcasted_iota(jnp.int32, (slots, width), 0).astype(F32)
        for d in range(step):
            late = j >= early_ref[d : d + 1, :]
            g = got[d * slots : (d + 1) * slots]
            out_ref[d * slots : (d + 1) * slots, :] = jnp.where(late, g[:, width:], g[:, :width]).astype(BF)

    return pl.pallas_call(
        body,
        grid=(groups // step,),
        in_specs=[
            pl.BlockSpec((step, tiles), lambda i: (i, 0)),
            pl.BlockSpec((step, width), lambda i: (i, 0)),
            pl.BlockSpec((tiles, width), lambda i: (0, 0)),
        ],
        out_specs=pl.BlockSpec((step * slots, width), lambda i: (i, 0)),
        out_shape=jax.ShapeDtypeStruct((groups * slots, width), BF),
        compiler_params=PARAMS,
        name="route",
    )(slot, early, table)


def cut_call(amplitudes, nx, nblk):
    owned, rows, full_width = amplitudes.shape
    sub = rows // nx
    width = full_width // nblk

    def body(a_ref, out_ref):
        for h in range(nx):
            for q in range(nblk):
                part = a_ref[:, h * sub : (h + 1) * sub, q * width : (q + 1) * width]
                out_ref[h * nblk + q] = jnp.swapaxes(part, 0, 1)

    return pl.pallas_call(
        body,
        grid=(1,),
        in_specs=[pl.BlockSpec(amplitudes.shape, lambda i: (0, 0, 0))],
        out_specs=pl.BlockSpec((nx * nblk, sub, owned, width), lambda i: (0, 0, 0, 0)),
        out_shape=jax.ShapeDtypeStruct((nx * nblk, sub, owned, width), BF),
        compiler_params=PARAMS,
        name="cut",
    )(amplitudes)


def turn_call(incoming, nblk, ny, nx, nz):
    depth, slots, width = incoming.shape
    step = 16
    low = ny // nblk

    def body(t_ref, out_ref):
        x = t_ref[...].reshape(nblk, low, nx, nz, step, width)
        order = [(b, y, h) for b in range(nblk) for h in range(nx) for y in range(low)]
        x = jnp.concatenate([x[b, y, h] for b, y, h in order], axis=0)
        x = jnp.swapaxes(x, 0, 1)
        for j in range(step):
            out_ref[j] = x[j].T

    return pl.pallas_call(
        body,
        grid=(slots // step,),
        in_specs=[pl.BlockSpec((depth, step, width), lambda i: (0, i, 0))],
        out_specs=pl.BlockSpec((step, width, depth), lambda i: (i, 0, 0)),
        out_shape=jax.ShapeDtypeStruct((slots, width, depth), BF),
        compiler_params=PARAMS,
        name="turn",
    )(incoming)


def ladder_call(slot, blk, flips, weights, turned, sources, occ, virt):
    columns, listed, depth, size = weights[0].shape
    width = turned.shape[1]
    owners = len(weights)
    some = 2

    def body(slot_ref, blk_ref, *refs):
        w_refs = refs[:owners]
        t_ref = refs[owners]
        s_refs = refs[owners + 1 : 2 * owners + 1]
        o_ref, v_ref, out_ref, held_ref, sems = refs[2 * owners + 1 :]
        for m in range(owners):
            for n in range(columns):
                at = m * columns + n
                pltpu.make_async_copy(w_refs[m].at[n], held_ref.at[at], sems.at[at]).start()
        for m in range(owners):
            to = blk_ref[0] ^ flips[m]

            def some_columns(i, _, m=m, to=to):
                for u in range(some):
                    n = i * some + u
                    at = m * columns + n
                    pltpu.make_async_copy(w_refs[m].at[n], held_ref.at[at], sems.at[at]).wait()
                    right, left = [], []
                    for r in range(listed):
                        s = slot_ref[at * listed + r]
                        w = held_ref[at, r]
                        hi = w.astype(BF)
                        lo = (w - hi.astype(F32)).astype(BF)
                        right.append(jnp.concatenate([hi, lo], axis=1))
                        t = t_ref[jnp.maximum(s, 0)]
                        left.append(jnp.where(s >= 0, t, jnp.zeros_like(t)))
                    right = jnp.concatenate(right, axis=0)
                    left = jnp.concatenate(left, axis=1)
                    acc = jnp.dot(left, right, preferred_element_type=F32)
                    part = (acc[:, :size] + acc[:, size:]).T
                    rows = pl.ds(n * size, size)
                    total = s_refs[m][rows, :].astype(F32) + part
                    v = jnp.broadcast_to(v_ref[pl.ds(at, 1), :], (size, size)).T
                    out_ref[to, rows, :] = (total / (v + o_ref[...])).astype(BF)
                return 0

            lax.fori_loop(0, columns // some, some_columns, 0)

    def whole(x):
        return pl.BlockSpec(x.shape, lambda i, s, b: (0,) * x.ndim)

    return pl.pallas_call(
        body,
        grid_spec=pltpu.PrefetchScalarGridSpec(
            num_scalar_prefetch=2,
            grid=(1,),
            in_specs=[pl.BlockSpec(memory_space=pl.ANY)] * owners
            + [whole(turned)]
            + [whole(x) for x in sources]
            + [pl.BlockSpec((1, width), lambda i, s, b: (0, b[0])), whole(virt)],
            out_specs=pl.BlockSpec((owners, columns * size, width), lambda i, s, b: (0, 0, 0)),
            scratch_shapes=[
                pltpu.VMEM((owners * columns, listed, depth, size), F32),
                pltpu.SemaphoreType.DMA((owners * columns,)),
            ],
        ),
        out_shape=jax.ShapeDtypeStruct((owners, columns * size, width), BF),
        compiler_params=pltpu.CompilerParams(vmem_limit_bytes=48 * 1024 * 1024),
        name="ladder",
    )(slot, blk, *weights, turned, *sources, occ, virt)


def swap(x, flip, n):
    return lax.ppermute(x, BLK, [(b, b ^ flip) for b in range(n)])


def per_device(amplitudes, integrals, tile_rows, destinations, source_terms, occ_energy, virt_energy):
    ny, nx, nz = (lax.axis_size(a) for a in GRP)
    nblk = lax.axis_size("xh") * lax.axis_size("k")
    groups = ny * nx * nz
    own = lax.axis_index(GRP).astype(jnp.int32)
    blk = lax.axis_index(BLK).astype(jnp.int32)
    owned, rows, full_width = amplitudes.shape
    all_tiles, dest = destinations.shape
    width = full_width // nblk
    sub = rows // nx
    slots = all_tiles * dest // groups
    columns, listed, _, size = integrals.shape

    x = cut_call(amplitudes, nx, nblk)
    x = lax.all_to_all(x, LINE, 0, 0, tiled=True)
    facts = [virt_energy.reshape(columns, size), tile_rows.astype(F32)]
    facts.append(jnp.zeros((columns, size - listed), F32))
    facts = jnp.concatenate(facts, axis=1)
    facts_across = swap(facts, 2, nblk)
    across = swap(integrals, 2, nblk)
    x = x.reshape(nx, nblk, sub, owned, width).transpose(1, 2, 0, 3, 4)
    x = lax.all_to_all(x.reshape(ny * nz, nx * owned, width), PLANE, 0, 0, tiled=True)
    table = x.reshape(all_tiles, width)

    dest_t = destinations.reshape(ny, nx, nz, owned, dest).transpose(4, 0, 2, 1, 3)
    slot_of, early, mine = rank_call(own.reshape(1), dest_t.reshape(dest, all_tiles), groups)
    outgoing = route_call(slot_of, early, table, slots)
    incoming = lax.all_to_all(outgoing.reshape(groups, slots, width), GRP, 0, 0, tiled=True)

    beside = swap(integrals, 1, nblk)
    facts = jnp.concatenate([facts, facts_across], axis=0)
    facts = jnp.concatenate([facts, swap(facts, 1, nblk)], axis=0)
    named_tiles = facts[:, size : size + listed].astype(jnp.int32)
    y_of = named_tiles // (nx * nz * owned)
    x_of = (named_tiles // (nz * owned)) % nx
    z_of = (named_tiles // owned) % nz
    at = ((y_of * nz + z_of) * nx + x_of) * owned + named_tiles % owned
    where = jnp.arange(all_tiles, dtype=jnp.int32)
    slot = jnp.max(jnp.where(at[:, :, None] == where, mine.reshape(1, 1, all_tiles), -1), axis=2)
    slot = slot.reshape(-1)
    diagonal = swap(across, 1, nblk)

    turned = turn_call(incoming, nblk, ny, nx, nz)

    def quarter(flip):
        return lax.dynamic_slice_in_dim(source_terms, (blk ^ flip) * width, width, 1)

    source_far = swap(quarter(2), 2, nblk)
    source_near = swap(quarter(1), 1, nblk)
    source_diagonal = swap(quarter(3), 3, nblk)

    done = ladder_call(
        slot,
        blk.reshape(1),
        (0, 2, 1, 3),
        (integrals, across, beside, diagonal),
        turned,
        (quarter(0), source_far, source_near, source_diagonal),
        occ_energy.reshape(1, full_width),
        facts[:, :size],
    )
    done = lax.all_to_all(done, BLK, 0, 0, tiled=True)
    return done.transpose(1, 0, 2).reshape(columns * size, full_width)


def solution(mesh):
    n_grp = mesh.shape["grp"]
    fine = Mesh(mesh.devices.reshape(8, 2, n_grp // 16, 2, 2), GRP + BLK)
    every = GRP + BLK
    in_specs = (
        P(GRP, BLK, None),
        P(every, None, None, None),
        P(every, None),
        P(),
        P(every, None),
        P(),
        P(every),
    )
    return jax.shard_map(
        per_device, mesh=fine, in_specs=in_specs, out_specs=P(every, None), check_vma=False
    )
```

```python
import jax
import jax.numpy as jnp
from jax import lax
from jax.experimental import pallas as pl
from jax.experimental.pallas import tpu as pltpu
from jax.sharding import Mesh, PartitionSpec as P


GRP = ("y", "xl", "z")
BLK = ("xh", "k")
LINE = ("xl", "xh", "k")
PLANE = ("y", "z")
BF = jnp.bfloat16
F32 = jnp.float32
PARAMS = pltpu.CompilerParams(vmem_limit_bytes=48 * 1024 * 1024)
WIDE = pltpu.CompilerParams(vmem_limit_bytes=46 * 1024 * 1024)
FULL = pltpu.CompilerParams(vmem_limit_bytes=67043328)


def rank_call(own, dest, groups):
    named_by, tiles = dest.shape
    lanes = 128
    half = tiles // 2 // lanes

    def body(own_ref, dest_ref, slot_ref, early_ref, mine_ref):
        ids = lax.broadcasted_iota(jnp.int32, (groups, lanes), 0)
        before = lax.broadcasted_iota(jnp.int32, (lanes, lanes), 0)
        after = lax.broadcasted_iota(jnp.int32, (lanes, lanes), 1)
        tri = (before < after).astype(F32).astype(BF)
        carry = jnp.zeros((groups, 1), F32)
        for i in range(tiles // lanes):
            if i == half:
                early_ref[...] = jnp.broadcast_to(carry, (groups, lanes))
            named = dest_ref[0:1, pl.ds(i * lanes, lanes)] == ids
            for l in range(1, named_by):
                named = named | (dest_ref[l : l + 1, pl.ds(i * lanes, lanes)] == ids)
            ones = named.astype(F32)
            earlier = jnp.dot(ones.astype(BF), tri, preferred_element_type=F32) + carry
            slot_ref[:, pl.ds(i * lanes, lanes)] = jnp.where(named, earlier, -1.0)
            carry = carry + jnp.sum(ones, axis=1, keepdims=True)
        mine_ref[...] = slot_ref[pl.ds(own_ref[0], 1), :].astype(jnp.int32)

    return pl.pallas_call(
        body,
        grid_spec=pltpu.PrefetchScalarGridSpec(
            num_scalar_prefetch=1,
            grid=(1,),
            in_specs=[pl.BlockSpec(dest.shape, lambda i, s: (0, 0))],
            out_specs=[
                pl.BlockSpec((groups, tiles), lambda i, s: (0, 0)),
                pl.BlockSpec((groups, lanes), lambda i, s: (0, 0)),
                pl.BlockSpec((1, tiles), lambda i, s: (0, 0)),
            ],
        ),
        out_shape=[
            jax.ShapeDtypeStruct((groups, tiles), F32),
            jax.ShapeDtypeStruct((groups, lanes), F32),
            jax.ShapeDtypeStruct((1, tiles), jnp.int32),
        ],
        compiler_params=PARAMS,
        name="rank",
    )(own, dest)


def route_call(slot, early, table, slots):
    groups, tiles = slot.shape
    width = table.shape[1]
    half = tiles // 2
    step = 32
    deep = 16

    def body(slot_ref, early_ref, table_ref, out_ref):
        one = jnp.asarray(1, BF)
        zero = jnp.asarray(0, BF)
        place = lax.broadcasted_iota(jnp.int32, (deep, half), 0)
        places = [(place + deep * q).astype(F32).astype(BF) for q in range(slots // deep)]
        rows = slot_ref[...]
        parts = []
        for d in range(step):
            lo = jnp.broadcast_to(rows[d : d + 1, :half], (deep, half)).astype(BF)
            hi = jnp.broadcast_to(rows[d : d + 1, half:], (deep, half)).astype(BF)
            for at in places:
                parts.append(jnp.where((lo == at) | (hi == at), one, zero))
        pick = jnp.concatenate(parts, axis=0)
        both = jnp.concatenate([table_ref[:half, :], table_ref[half:, :]], axis=1)
        got = jnp.dot(pick, both, preferred_element_type=F32)
        j = lax.broadcasted_iota(jnp.int32, (slots, width), 0).astype(F32)
        for d in range(step):
            late = j >= early_ref[d : d + 1, :]
            g = got[d * slots : (d + 1) * slots]
            out_ref[d * slots : (d + 1) * slots, :] = jnp.where(late, g[:, width:], g[:, :width]).astype(BF)

    return pl.pallas_call(
        body,
        grid=(groups // step,),
        in_specs=[
            pl.BlockSpec((step, tiles), lambda i: (i, 0)),
            pl.BlockSpec((step, width), lambda i: (i, 0)),
            pl.BlockSpec((tiles, width), lambda i: (0, 0)),
        ],
        out_specs=pl.BlockSpec((step * slots, width), lambda i: (i, 0)),
        out_shape=jax.ShapeDtypeStruct((groups * slots, width), BF),
        compiler_params=PARAMS,
        name="route",
    )(slot, early, table)


def cut_call(amplitudes, nx, nblk):
    owned, rows, full_width = amplitudes.shape
    sub = rows // nx
    width = full_width // nblk

    def body(a_ref, out_ref, held_ref, sems):
        def load(q):
            part = a_ref.at[:, :, pl.ds(q * width, width)]
            return pltpu.make_async_copy(part, held_ref.at[q], sems.at[q])

        for q in range(nblk):
            load(q).start()
        for q in range(nblk):
            load(q).wait()
            for h in range(nx):
                out_ref[h * nblk + q] = jnp.swapaxes(held_ref[q, :, h * sub : (h + 1) * sub, :], 0, 1)

    return pl.pallas_call(
        body,
        grid=(1,),
        in_specs=[pl.BlockSpec(memory_space=pl.ANY)],
        out_specs=pl.BlockSpec((nx * nblk, sub, owned, width), lambda i: (0, 0, 0, 0)),
        out_shape=jax.ShapeDtypeStruct((nx * nblk, sub, owned, width), BF),
        scratch_shapes=[
            pltpu.VMEM((nblk, owned, rows, width), BF),
            pltpu.SemaphoreType.DMA((nblk,)),
        ],
        compiler_params=FULL,
        name="cut",
    )(amplitudes)


def turn_call(incoming, nblk, ny, nx, nz):
    depth, slots, width = incoming.shape
    step = 16
    low = ny // nblk

    def body(t_ref, out_ref):
        x = t_ref[...].reshape(nblk, low, nx, nz, step, width)
        order = [(b, y, h) for b in range(nblk) for h in range(nx) for y in range(low)]
        x = jnp.concatenate([x[b, y, h] for b, y, h in order], axis=0)
        x = jnp.swapaxes(x, 0, 1)
        for j in range(step):
            out_ref[j] = x[j].T

    return pl.pallas_call(
        body,
        grid=(slots // step,),
        in_specs=[pl.BlockSpec((depth, step, width), lambda i: (0, i, 0))],
        out_specs=pl.BlockSpec((step, width, depth), lambda i: (i, 0, 0)),
        out_shape=jax.ShapeDtypeStruct((slots, width, depth), BF),
        compiler_params=PARAMS,
        name="turn",
    )(incoming)


def ladder_call(slot, blk, first, weights, turned, sources, occ, virt, ready=None, places=None):
    columns, listed, depth, size = weights[0].shape
    width = turned.shape[1]
    owners = len(weights)
    some = 2
    total = owners if places is None else len(places)

    def body(slot_ref, blk_ref, *refs):
        w_refs = refs[:owners]
        t_ref = refs[owners]
        s_refs = refs[owners + 1 : 2 * owners + 1]
        o_ref, v_ref = refs[2 * owners + 1 : 2 * owners + 3]
        out_ref, held_ref, sems = refs[-3:]
        for m in range(owners):
            for n in range(columns):
                at = m * columns + n
                pltpu.make_async_copy(w_refs[m].at[n], held_ref.at[at], sems.at[at]).start()
        if places is not None:
            for m in range(first):
                out_ref[blk_ref[0] ^ places[m]] = refs[-4][m]
        for m in range(owners):
            to = m if places is None else blk_ref[0] ^ places[first + m]

            def some_columns(i, _, m=m, to=to):
                for u in range(some):
                    n = i * some + u
                    at = m * columns + n
                    named = first * columns + at
                    pltpu.make_async_copy(w_refs[m].at[n], held_ref.at[at], sems.at[at]).wait()
                    right, left = [], []
                    for r in range(listed):
                        s = slot_ref[named * listed + r]
                        w = held_ref[at, r]
                        hi = w.astype(BF)
                        lo = (w - hi.astype(F32)).astype(BF)
                        right.append(jnp.concatenate([hi, lo], axis=1))
                        t = t_ref[jnp.maximum(s, 0)]
                        left.append(jnp.where(s >= 0, t, jnp.zeros_like(t)))
                    right = jnp.concatenate(right, axis=0)
                    left = jnp.concatenate(left, axis=1)
                    acc = jnp.dot(left, right, preferred_element_type=F32)
                    part = (acc[:, :size] + acc[:, size:]).T
                    rows = pl.ds(n * size, size)
                    summed = s_refs[m][rows, :].astype(F32) + part
                    v = jnp.broadcast_to(v_ref[pl.ds(named, 1), :], (size, size)).T
                    out_ref[to, rows, :] = (summed / (v + o_ref[...])).astype(BF)
                return 0

            lax.fori_loop(0, columns // some, some_columns, 0)

    def whole(x):
        return pl.BlockSpec(x.shape, lambda i, s, b: (0,) * x.ndim)

    extra = () if ready is None else (ready,)
    return pl.pallas_call(
        body,
        grid_spec=pltpu.PrefetchScalarGridSpec(
            num_scalar_prefetch=2,
            grid=(1,),
            in_specs=[pl.BlockSpec(memory_space=pl.ANY)] * owners
            + [whole(turned)]
            + [whole(x) for x in sources]
            + [pl.BlockSpec((1, width), lambda i, s, b: (0, b[0])), whole(virt)]
            + [whole(x) for x in extra],
            out_specs=pl.BlockSpec((total, columns * size, width), lambda i, s, b: (0, 0, 0)),
            scratch_shapes=[
                pltpu.VMEM((owners * columns, listed, depth, size), F32),
                pltpu.SemaphoreType.DMA((owners * columns,)),
            ],
        ),
        out_shape=jax.ShapeDtypeStruct((total, columns * size, width), BF),
        compiler_params=WIDE,
        name="ladder",
    )(slot, blk, *weights, turned, *sources, occ, virt, *extra)


def swap(x, flip, n):
    return lax.ppermute(x, BLK, [(b, b ^ flip) for b in range(n)])


def per_device(amplitudes, integrals, tile_rows, destinations, source_terms, occ_energy, virt_energy):
    ny, nx, nz = (lax.axis_size(a) for a in GRP)
    nblk = lax.axis_size("xh") * lax.axis_size("k")
    groups = ny * nx * nz
    own = lax.axis_index(GRP).astype(jnp.int32)
    blk = lax.axis_index(BLK).astype(jnp.int32)
    owned, rows, full_width = amplitudes.shape
    all_tiles, dest = destinations.shape
    width = full_width // nblk
    sub = rows // nx
    slots = all_tiles * dest // groups
    columns, listed, _, size = integrals.shape

    x = cut_call(amplitudes, nx, nblk)
    x = lax.all_to_all(x, LINE, 0, 0, tiled=True)
    facts = [virt_energy.reshape(columns, size), tile_rows.astype(F32)]
    facts.append(jnp.zeros((columns, size - listed), F32))
    facts = jnp.concatenate(facts, axis=1)
    facts_across = swap(facts, 2, nblk)
    across = swap(integrals, 2, nblk)
    x = x.reshape(nx, nblk, sub, owned, width).transpose(1, 2, 0, 3, 4)
    x = lax.all_to_all(x.reshape(ny * nz, nx * owned, width), PLANE, 0, 0, tiled=True)
    table = x.reshape(all_tiles, width)

    dest_t = destinations.reshape(ny, nx, nz, owned, dest).transpose(4, 0, 2, 1, 3)
    slot_of, early, mine = rank_call(own.reshape(1), dest_t.reshape(dest, all_tiles), groups)
    outgoing = route_call(slot_of, early, table, slots)
    incoming = lax.all_to_all(outgoing.reshape(groups, slots, width), GRP, 0, 0, tiled=True)

    beside = swap(integrals, 1, nblk)
    pair = jnp.concatenate([facts, facts_across], axis=0)
    other = swap(pair, 1, nblk)
    facts = jnp.concatenate([facts, other[:columns], facts_across, other[columns:]], axis=0)
    named_tiles = facts[:, size : size + listed].astype(jnp.int32)
    y_of = named_tiles // (nx * nz * owned)
    x_of = (named_tiles // (nz * owned)) % nx
    z_of = (named_tiles // owned) % nz
    at = ((y_of * nz + z_of) * nx + x_of) * owned + named_tiles % owned
    where = jnp.arange(all_tiles, dtype=jnp.int32)
    slot = jnp.max(jnp.where(at[:, :, None] == where, mine.reshape(1, 1, all_tiles), -1), axis=2)
    slot = slot.reshape(-1)
    diagonal = swap(across, 1, nblk)

    turned = turn_call(incoming, nblk, ny, nx, nz)

    def quarter(flip):
        return lax.dynamic_slice_in_dim(source_terms, (blk ^ flip) * width, width, 1)

    source_far = swap(quarter(2), 2, nblk)
    source_near = swap(quarter(1), 1, nblk)
    source_diagonal = swap(quarter(3), 3, nblk)

    occ = occ_energy.reshape(1, full_width)
    virt = facts[:, :size]
    mine = blk.reshape(1)
    local = ladder_call(
        slot, mine, 0, (integrals, beside), turned, (quarter(0), source_near), occ, virt
    )
    done = ladder_call(
        slot,
        mine,
        2,
        (across, diagonal),
        turned,
        (source_far, source_diagonal),
        occ,
        virt,
        ready=local,
        places=(0, 1, 2, 3),
    )
    done = lax.all_to_all(done, BLK, 0, 0, tiled=True)
    return done.transpose(1, 0, 2).reshape(columns * size, full_width)


def solution(mesh):
    n_grp = mesh.shape["grp"]
    fine = Mesh(mesh.devices.reshape(8, 2, n_grp // 16, 2, 2), GRP + BLK)
    every = GRP + BLK
    in_specs = (
        P(GRP, BLK, None),
        P(every, None, None, None),
        P(every, None),
        P(),
        P(every, None),
        P(),
        P(every),
    )
    return jax.shard_map(per_device, mesh=fine, in_specs=in_specs, out_specs=P(every, None), check_vma=False)
```

```python
import jax
import jax.numpy as jnp
from jax import lax
from jax.experimental import pallas as pl
from jax.experimental.pallas import tpu as pltpu
from jax.sharding import Mesh, PartitionSpec as P


GRP = ("y", "xl", "z")
BLK = ("xh", "k")
LINE = ("xl", "xh", "k")
PLANE = ("y", "z")
BF = jnp.bfloat16
F32 = jnp.float32
PARAMS = pltpu.CompilerParams(vmem_limit_bytes=48 * 1024 * 1024)
FULL = pltpu.CompilerParams(vmem_limit_bytes=67043328)


def rank_call(own, dest, groups):
    named_by, tiles = dest.shape
    lanes = 128
    half = tiles // 2 // lanes

    def body(own_ref, dest_ref, slot_ref, early_ref, mine_ref):
        ids = lax.broadcasted_iota(jnp.int32, (groups, lanes), 0)
        before = lax.broadcasted_iota(jnp.int32, (lanes, lanes), 0)
        after = lax.broadcasted_iota(jnp.int32, (lanes, lanes), 1)
        tri = (before < after).astype(F32).astype(BF)
        carry = jnp.zeros((groups, 1), F32)
        for i in range(tiles // lanes):
            if i == half:
                early_ref[...] = jnp.broadcast_to(carry, (groups, lanes))
            named = dest_ref[0:1, pl.ds(i * lanes, lanes)] == ids
            for l in range(1, named_by):
                named = named | (dest_ref[l : l + 1, pl.ds(i * lanes, lanes)] == ids)
            ones = named.astype(F32)
            earlier = jnp.dot(ones.astype(BF), tri, preferred_element_type=F32) + carry
            slot_ref[:, pl.ds(i * lanes, lanes)] = jnp.where(named, earlier, -1.0)
            carry = carry + jnp.sum(ones, axis=1, keepdims=True)
        mine_ref[...] = slot_ref[pl.ds(own_ref[0], 1), :].astype(jnp.int32)

    return pl.pallas_call(
        body,
        grid_spec=pltpu.PrefetchScalarGridSpec(
            num_scalar_prefetch=1,
            grid=(1,),
            in_specs=[pl.BlockSpec(dest.shape, lambda i, s: (0, 0))],
            out_specs=[
                pl.BlockSpec((groups, tiles), lambda i, s: (0, 0)),
                pl.BlockSpec((groups, lanes), lambda i, s: (0, 0)),
                pl.BlockSpec((1, tiles), lambda i, s: (0, 0)),
            ],
        ),
        out_shape=[
            jax.ShapeDtypeStruct((groups, tiles), F32),
            jax.ShapeDtypeStruct((groups, lanes), F32),
            jax.ShapeDtypeStruct((1, tiles), jnp.int32),
        ],
        compiler_params=PARAMS,
        name="rank",
    )(own, dest)


def route_call(slot, early, table, slots):
    groups, tiles = slot.shape
    width = table.shape[1]
    half = tiles // 2
    step = 32
    deep = 16

    def body(slot_ref, early_ref, table_ref, out_ref):
        one = jnp.asarray(1, BF)
        zero = jnp.asarray(0, BF)
        place = lax.broadcasted_iota(jnp.int32, (deep, half), 0)
        places = [(place + deep * q).astype(F32).astype(BF) for q in range(slots // deep)]
        rows = slot_ref[...]
        parts = []
        for d in range(step):
            lo = jnp.broadcast_to(rows[d : d + 1, :half], (deep, half)).astype(BF)
            hi = jnp.broadcast_to(rows[d : d + 1, half:], (deep, half)).astype(BF)
            for at in places:
                parts.append(jnp.where((lo == at) | (hi == at), one, zero))
        pick = jnp.concatenate(parts, axis=0)
        both = jnp.concatenate([table_ref[:half, :], table_ref[half:, :]], axis=1)
        got = jnp.dot(pick, both, preferred_element_type=F32)
        j = lax.broadcasted_iota(jnp.int32, (slots, width), 0).astype(F32)
        for d in range(step):
            late = j >= early_ref[d : d + 1, :]
            g = got[d * slots : (d + 1) * slots]
            out_ref[d * slots : (d + 1) * slots, :] = jnp.where(late, g[:, width:], g[:, :width]).astype(BF)

    return pl.pallas_call(
        body,
        grid=(groups // step,),
        in_specs=[
            pl.BlockSpec((step, tiles), lambda i: (i, 0)),
            pl.BlockSpec((step, width), lambda i: (i, 0)),
            pl.BlockSpec((tiles, width), lambda i: (0, 0)),
        ],
        out_specs=pl.BlockSpec((step * slots, width), lambda i: (i, 0)),
        out_shape=jax.ShapeDtypeStruct((groups * slots, width), BF),
        compiler_params=PARAMS,
        name="route",
    )(slot, early, table)


def cut_call(amplitudes, virt, tile_rows, nx, nblk):
    owned, rows, full_width = amplitudes.shape
    sub = rows // nx
    width = full_width // nblk
    columns, listed = tile_rows.shape

    def body(a_ref, v_ref, r_ref, out_ref, held_ref, virt_ref, rows_ref, slab_ref, sems):
        facts = (
            pltpu.make_async_copy(v_ref, virt_ref, sems.at[nblk]),
            pltpu.make_async_copy(r_ref, rows_ref, sems.at[nblk + 1]),
        )

        def load(q):
            part = a_ref.at[:, :, pl.ds(q * width, width)]
            return pltpu.make_async_copy(part, held_ref.at[q], sems.at[q])

        for fact in facts:
            fact.start()
        for q in range(nblk):
            load(q).start()
        slab_ref[...] = jnp.zeros((owned, width), F32)
        for fact in facts:
            fact.wait()
        left = virt_ref[...]
        for i in range(3):
            part = left.astype(BF).astype(F32)
            slab_ref[i * columns : (i + 1) * columns, :] = part
            left = left - part
        last = slice(3 * columns, 4 * columns)
        slab_ref[last, 0:listed] = (rows_ref[...] >> 6).astype(F32)
        slab_ref[last, listed : 2 * listed] = (rows_ref[...] & 63).astype(F32)
        slab = slab_ref[...].astype(BF)
        for q in range(nblk):
            load(q).wait()
            for h in range(nx):
                part = held_ref[q, :, h * sub : (h + 1) * sub, :]
                out_ref[h * nblk + q, :sub] = jnp.swapaxes(part, 0, 1)
                out_ref[h * nblk + q, sub] = slab

    return pl.pallas_call(
        body,
        grid=(1,),
        in_specs=[pl.BlockSpec(memory_space=pl.ANY)] * 3,
        out_specs=pl.BlockSpec((nx * nblk, sub + 1, owned, width), lambda i: (0, 0, 0, 0)),
        out_shape=jax.ShapeDtypeStruct((nx * nblk, sub + 1, owned, width), BF),
        scratch_shapes=[
            pltpu.VMEM((nblk, owned, rows, width), BF),
            pltpu.VMEM(virt.shape, F32),
            pltpu.VMEM(tile_rows.shape, jnp.int32),
            pltpu.VMEM((owned, width), F32),
            pltpu.SemaphoreType.DMA((nblk + 2,)),
        ],
        compiler_params=FULL,
        name="cut",
    )(amplitudes, virt, tile_rows)


def turn_call(incoming, nblk, ny, nx, nz):
    depth, slots, width = incoming.shape
    step = 16
    low = ny // nblk

    def body(t_ref, out_ref):
        x = t_ref[...].reshape(nblk, low, nx, nz, step, width)
        order = [(b, y, h) for b in range(nblk) for h in range(nx) for y in range(low)]
        x = jnp.concatenate([x[b, y, h] for b, y, h in order], axis=0)
        x = jnp.swapaxes(x, 0, 1)
        for j in range(step):
            out_ref[j] = x[j].T

    return pl.pallas_call(
        body,
        grid=(slots // step,),
        in_specs=[pl.BlockSpec((depth, step, width), lambda i: (0, i, 0))],
        out_specs=pl.BlockSpec((step, width, depth), lambda i: (i, 0, 0)),
        out_shape=jax.ShapeDtypeStruct((slots, width, depth), BF),
        compiler_params=PARAMS,
        name="turn",
    )(incoming)


def ladder_call(slot, blk, flips, weights, turned, sources, occ, virt, ready=None, before=()):
    columns, listed, depth, size = weights[0].shape
    width = turned.shape[1]
    owners = len(weights)
    some = 2
    total = owners + len(before)

    def body(slot_ref, blk_ref, *refs):
        w_refs = refs[:owners]
        t_ref = refs[owners]
        s_refs = refs[owners + 1 : 2 * owners + 1]
        o_ref, v_ref = refs[2 * owners + 1 : 2 * owners + 3]
        out_ref, held_ref, sems = refs[-3:]
        for m in range(owners):
            for n in range(columns):
                at = m * columns + n
                pltpu.make_async_copy(w_refs[m].at[n], held_ref.at[at], sems.at[at]).start()
        for m, flip in enumerate(before):
            out_ref[blk_ref[0] ^ flip] = refs[-4][m]
        for m in range(owners):
            owner = blk_ref[0] ^ flips[m]
            to = owner if before else m

            def some_columns(i, _, m=m, to=to, owner=owner):
                for u in range(some):
                    n = i * some + u
                    at = m * columns + n
                    named = owner * columns + n
                    pltpu.make_async_copy(w_refs[m].at[n], held_ref.at[at], sems.at[at]).wait()
                    right, left = [], []
                    for r in range(listed):
                        s = slot_ref[named * listed + r]
                        w = held_ref[at, r]
                        hi = w.astype(BF)
                        lo = (w - hi.astype(F32)).astype(BF)
                        right.append(jnp.concatenate([hi, lo], axis=1))
                        t = t_ref[jnp.maximum(s, 0)]
                        left.append(jnp.where(s >= 0, t, jnp.zeros_like(t)))
                    right = jnp.concatenate(right, axis=0)
                    left = jnp.concatenate(left, axis=1)
                    acc = jnp.dot(left, right, preferred_element_type=F32)
                    part = (acc[:, :size] + acc[:, size:]).T
                    rows = pl.ds(n * size, size)
                    summed = s_refs[m][rows, :].astype(F32) + part
                    v = jnp.broadcast_to(v_ref[pl.ds(named, 1), :], (size, size)).T
                    out_ref[to, rows, :] = (summed / (v + o_ref[...])).astype(BF)
                return 0

            lax.fori_loop(0, columns // some, some_columns, 0)

    def whole(x):
        return pl.BlockSpec(x.shape, lambda i, s, b: (0,) * x.ndim)

    extra = () if ready is None else (ready,)
    return pl.pallas_call(
        body,
        grid_spec=pltpu.PrefetchScalarGridSpec(
            num_scalar_prefetch=2,
            grid=(1,),
            in_specs=[pl.BlockSpec(memory_space=pl.ANY)] * owners
            + [whole(turned)]
            + [whole(x) for x in sources]
            + [pl.BlockSpec((1, width), lambda i, s, b: (0, b[0])), whole(virt)]
            + [whole(x) for x in extra],
            out_specs=pl.BlockSpec((total, columns * size, width), lambda i, s, b: (0, 0, 0)),
            scratch_shapes=[
                pltpu.VMEM((owners * columns, listed, depth, size), F32),
                pltpu.SemaphoreType.DMA((owners * columns,)),
            ],
        ),
        out_shape=jax.ShapeDtypeStruct((total, columns * size, width), BF),
        compiler_params=PARAMS,
        name="ladder",
    )(slot, blk, *weights, turned, *sources, occ, virt, *extra)


def swap(x, flip, n):
    return lax.ppermute(x, BLK, [(b, b ^ flip) for b in range(n)])


def per_device(amplitudes, integrals, tile_rows, destinations, source_terms, occ_energy, virt_energy):
    ny, nx, nz = (lax.axis_size(a) for a in GRP)
    nblk = lax.axis_size("xh") * lax.axis_size("k")
    groups = ny * nx * nz
    own = lax.axis_index(GRP).astype(jnp.int32)
    blk = lax.axis_index(BLK).astype(jnp.int32)
    owned, rows, full_width = amplitudes.shape
    all_tiles, dest = destinations.shape
    width = full_width // nblk
    sub = rows // nx
    slots = all_tiles * dest // groups
    columns, listed, _, size = integrals.shape

    x = cut_call(amplitudes, virt_energy.reshape(columns, size), tile_rows, nx, nblk)
    x = lax.all_to_all(x, LINE, 0, 0, tiled=True)
    across = swap(integrals, 2, nblk)
    slabs = x[:, sub].reshape(nx, nblk, owned, width)
    x = x[:, :sub].reshape(nx, nblk, sub, owned, width).transpose(1, 2, 0, 3, 4)
    x = lax.all_to_all(x.reshape(ny * nz, nx * owned, width), PLANE, 0, 0, tiled=True)
    table = x.reshape(all_tiles, width)

    dest_t = destinations.reshape(ny, nx, nz, owned, dest).transpose(4, 0, 2, 1, 3)
    slot_of, early, mine = rank_call(own.reshape(1), dest_t.reshape(dest, all_tiles), groups)
    outgoing = route_call(slot_of, early, table, slots)
    incoming = lax.all_to_all(outgoing.reshape(groups, slots, width), GRP, 0, 0, tiled=True)

    beside = swap(integrals, 1, nblk)
    slab = lax.dynamic_index_in_dim(slabs, lax.axis_index("xl"), 0, keepdims=False)
    slab = slab.astype(F32).reshape(nblk, 4, columns, width)
    virt = (slab[:, 0] + slab[:, 1] + slab[:, 2]).reshape(nblk * columns, size)
    named_tiles = slab[:, 3, :, :listed] * 64 + slab[:, 3, :, listed : 2 * listed]
    named_tiles = named_tiles.astype(jnp.int32).reshape(nblk * columns, listed)
    y_of = named_tiles // (nx * nz * owned)
    x_of = (named_tiles // (nz * owned)) % nx
    z_of = (named_tiles // owned) % nz
    at = ((y_of * nz + z_of) * nx + x_of) * owned + named_tiles % owned
    where = jnp.arange(all_tiles, dtype=jnp.int32)
    slot = jnp.max(jnp.where(at[:, :, None] == where, mine.reshape(1, 1, all_tiles), -1), axis=2)
    slot = slot.reshape(-1)
    diagonal = swap(across, 1, nblk)

    turned = turn_call(incoming, nblk, ny, nx, nz)

    def quarter(flip):
        return lax.dynamic_slice_in_dim(source_terms, (blk ^ flip) * width, width, 1)

    source_far = swap(quarter(2), 2, nblk)
    source_near = swap(quarter(1), 1, nblk)
    source_diagonal = swap(quarter(3), 3, nblk)

    occ = occ_energy.reshape(1, full_width)
    mine = blk.reshape(1)
    local = ladder_call(
        slot, mine, (0, 1), (integrals, beside), turned, (quarter(0), source_near), occ, virt
    )
    done = ladder_call(
        slot,
        mine,
        (2, 3),
        (across, diagonal),
        turned,
        (source_far, source_diagonal),
        occ,
        virt,
        ready=local,
        before=(0, 1),
    )
    done = lax.all_to_all(done, BLK, 0, 0, tiled=True)
    return done.transpose(1, 0, 2).reshape(columns * size, full_width)


def solution(mesh):
    n_grp = mesh.shape["grp"]
    fine = Mesh(mesh.devices.reshape(8, 2, n_grp // 16, 2, 2), GRP + BLK)
    every = GRP + BLK
    in_specs = (
        P(GRP, BLK, None),
        P(every, None, None, None),
        P(every, None),
        P(),
        P(every, None),
        P(),
        P(every),
    )
    return jax.shard_map(
        per_device, mesh=fine, in_specs=in_specs, out_specs=P(every, None), check_vma=False
    )
```

```python
import jax
import jax.numpy as jnp
from jax import lax
from jax.experimental import pallas as pl
from jax.experimental.pallas import tpu as pltpu
from jax.sharding import Mesh, PartitionSpec as P


GRP = ("y", "xl", "z")
BLK = ("xh", "k")
LINE = ("xl", "xh", "k")
PLANE = ("y", "z")
BF = jnp.bfloat16
F32 = jnp.float32
PARAMS = pltpu.CompilerParams(vmem_limit_bytes=48 * 1024 * 1024)


def quarter_of(x_lo, b):
    return b ^ ((x_lo & b & 1) << 1)


def rank_call(own, dest, groups):
    named_by, tiles = dest.shape
    lanes = 128
    half = tiles // 2 // lanes

    def body(own_ref, dest_ref, slot_ref, early_ref, mine_ref):
        ids = lax.broadcasted_iota(jnp.int32, (groups, lanes), 0)
        before = lax.broadcasted_iota(jnp.int32, (lanes, lanes), 0)
        after = lax.broadcasted_iota(jnp.int32, (lanes, lanes), 1)
        tri = (before < after).astype(F32).astype(BF)
        carry = jnp.zeros((groups, 1), F32)
        for i in range(tiles // lanes):
            if i == half:
                early_ref[...] = jnp.broadcast_to(carry, (groups, lanes))
            named = dest_ref[0:1, pl.ds(i * lanes, lanes)] == ids
            for l in range(1, named_by):
                named = named | (dest_ref[l : l + 1, pl.ds(i * lanes, lanes)] == ids)
            ones = named.astype(F32)
            earlier = jnp.dot(ones.astype(BF), tri, preferred_element_type=F32) + carry
            slot_ref[:, pl.ds(i * lanes, lanes)] = jnp.where(named, earlier, -1.0)
            carry = carry + jnp.sum(ones, axis=1, keepdims=True)
        mine_ref[...] = slot_ref[pl.ds(own_ref[0], 1), :].astype(jnp.int32)

    return pl.pallas_call(
        body,
        grid_spec=pltpu.PrefetchScalarGridSpec(
            num_scalar_prefetch=1,
            grid=(1,),
            in_specs=[pl.BlockSpec(dest.shape, lambda i, s: (0, 0))],
            out_specs=[
                pl.BlockSpec((groups, tiles), lambda i, s: (0, 0)),
                pl.BlockSpec((groups, lanes), lambda i, s: (0, 0)),
                pl.BlockSpec((1, tiles), lambda i, s: (0, 0)),
            ],
        ),
        out_shape=[
            jax.ShapeDtypeStruct((groups, tiles), F32),
            jax.ShapeDtypeStruct((groups, lanes), F32),
            jax.ShapeDtypeStruct((1, tiles), jnp.int32),
        ],
        compiler_params=PARAMS,
        name="rank",
    )(own, dest)


def route_call(slot, early, table, slots):
    groups, tiles = slot.shape
    width = table.shape[1]
    half = tiles // 2
    step = 32
    deep = 16

    def body(slot_ref, early_ref, table_ref, out_ref):
        one = jnp.asarray(1, BF)
        zero = jnp.asarray(0, BF)
        place = lax.broadcasted_iota(jnp.int32, (deep, half), 0)
        places = [(place + deep * q).astype(F32).astype(BF) for q in range(slots // deep)]
        rows = slot_ref[...]
        parts = []
        for d in range(step):
            lo = jnp.broadcast_to(rows[d : d + 1, :half], (deep, half)).astype(BF)
            hi = jnp.broadcast_to(rows[d : d + 1, half:], (deep, half)).astype(BF)
            for at in places:
                parts.append(jnp.where((lo == at) | (hi == at), one, zero))
        pick = jnp.concatenate(parts, axis=0)
        both = jnp.concatenate([table_ref[:half, :], table_ref[half:, :]], axis=1)
        got = jnp.dot(pick, both, preferred_element_type=F32)
        j = lax.broadcasted_iota(jnp.int32, (slots, width), 0).astype(F32)
        for d in range(step):
            late = j >= early_ref[d : d + 1, :]
            g = got[d * slots : (d + 1) * slots]
            out_ref[d * slots : (d + 1) * slots, :] = jnp.where(late, g[:, width:], g[:, :width]).astype(BF)

    return pl.pallas_call(
        body,
        grid=(groups // step,),
        in_specs=[
            pl.BlockSpec((step, tiles), lambda i: (i, 0)),
            pl.BlockSpec((step, width), lambda i: (i, 0)),
            pl.BlockSpec((tiles, width), lambda i: (0, 0)),
        ],
        out_specs=pl.BlockSpec((step * slots, width), lambda i: (i, 0)),
        out_shape=jax.ShapeDtypeStruct((groups * slots, width), BF),
        compiler_params=PARAMS,
        name="route",
    )(slot, early, table)


def cut_call(amplitudes, nx, nblk):
    owned, rows, full_width = amplitudes.shape
    sub = rows // nx
    width = full_width // nblk

    def body(a_ref, out_ref):
        for h in range(nx):
            for q in range(nblk):
                part = a_ref[:, h * sub : (h + 1) * sub, q * width : (q + 1) * width]
                out_ref[h * nblk + quarter_of(h, q)] = jnp.swapaxes(part, 0, 1)

    return pl.pallas_call(
        body,
        grid=(1,),
        in_specs=[pl.BlockSpec(amplitudes.shape, lambda i: (0, 0, 0))],
        out_specs=pl.BlockSpec((nx * nblk, sub, owned, width), lambda i: (0, 0, 0, 0)),
        out_shape=jax.ShapeDtypeStruct((nx * nblk, sub, owned, width), BF),
        compiler_params=PARAMS,
        name="cut",
    )(amplitudes)


def turn_call(incoming, nblk, ny, nx, nz):
    depth, slots, width = incoming.shape
    step = 16
    low = ny // nblk

    def body(t_ref, out_ref):
        x = t_ref[...].reshape(nblk, low, nx, nz, step, width)
        order = [(b, y, h) for b in range(nblk) for h in range(nx) for y in range(low)]
        x = jnp.concatenate([x[b, y, h] for b, y, h in order], axis=0)
        x = jnp.swapaxes(x, 0, 1)
        for j in range(step):
            out_ref[j] = x[j].T

    return pl.pallas_call(
        body,
        grid=(slots // step,),
        in_specs=[pl.BlockSpec((depth, step, width), lambda i: (0, i, 0))],
        out_specs=pl.BlockSpec((step, width, depth), lambda i: (i, 0, 0)),
        out_shape=jax.ShapeDtypeStruct((slots, width, depth), BF),
        compiler_params=PARAMS,
        name="turn",
    )(incoming)


def ladder_call(slot, blk, first, weights, turned, sources, occ, virt, ready=None, places=None):
    columns, listed, depth, size = weights[0].shape
    width = turned.shape[1]
    owners = len(weights)
    some = 2
    total = owners if places is None else len(places)

    def body(slot_ref, blk_ref, *refs):
        w_refs = refs[:owners]
        t_ref = refs[owners]
        s_refs = refs[owners + 1 : 2 * owners + 1]
        o_ref, v_ref = refs[2 * owners + 1 : 2 * owners + 3]
        out_ref, held_ref, sems = refs[-3:]
        for m in range(owners):
            for n in range(columns):
                at = m * columns + n
                pltpu.make_async_copy(w_refs[m].at[n], held_ref.at[at], sems.at[at]).start()
        if places is not None:
            for m in range(first):
                out_ref[blk_ref[0] ^ places[m]] = refs[-4][m]
        for m in range(owners):
            to = m if places is None else blk_ref[0] ^ places[first + m]

            def some_columns(i, _, m=m, to=to):
                for u in range(some):
                    n = i * some + u
                    at = m * columns + n
                    named = first * columns + at
                    pltpu.make_async_copy(w_refs[m].at[n], held_ref.at[at], sems.at[at]).wait()
                    right, left = [], []
                    for r in range(listed):
                        s = slot_ref[named * listed + r]
                        w = held_ref[at, r]
                        hi = w.astype(BF)
                        lo = (w - hi.astype(F32)).astype(BF)
                        right.append(jnp.concatenate([hi, lo], axis=1))
                        t = t_ref[jnp.maximum(s, 0)]
                        left.append(jnp.where(s >= 0, t, jnp.zeros_like(t)))
                    right = jnp.concatenate(right, axis=0)
                    left = jnp.concatenate(left, axis=1)
                    acc = jnp.dot(left, right, preferred_element_type=F32)
                    part = (acc[:, :size] + acc[:, size:]).T
                    rows = pl.ds(n * size, size)
                    summed = s_refs[m][rows, :].astype(F32) + part
                    v = jnp.broadcast_to(v_ref[pl.ds(named, 1), :], (size, size)).T
                    out_ref[to, rows, :] = (summed / (v + o_ref[...])).astype(BF)
                return 0

            lax.fori_loop(0, columns // some, some_columns, 0)

    def whole(x):
        return pl.BlockSpec(x.shape, lambda i, s, b: (0,) * x.ndim)

    extra = () if ready is None else (ready,)
    return pl.pallas_call(
        body,
        grid_spec=pltpu.PrefetchScalarGridSpec(
            num_scalar_prefetch=2,
            grid=(1,),
            in_specs=[pl.BlockSpec(memory_space=pl.ANY)] * owners
            + [whole(turned)]
            + [whole(x) for x in sources]
            + [pl.BlockSpec((1, width), lambda i, s, b: (0, b[1])), whole(virt)]
            + [whole(x) for x in extra],
            out_specs=pl.BlockSpec((total, columns * size, width), lambda i, s, b: (0, 0, 0)),
            scratch_shapes=[
                pltpu.VMEM((owners * columns, listed, depth, size), F32),
                pltpu.SemaphoreType.DMA((owners * columns,)),
            ],
        ),
        out_shape=jax.ShapeDtypeStruct((total, columns * size, width), BF),
        compiler_params=PARAMS,
        name="ladder",
    )(slot, blk, *weights, turned, *sources, occ, virt, *extra)


def swap(x, flip, n):
    return lax.ppermute(x, BLK, [(b, b ^ flip) for b in range(n)])


def per_device(amplitudes, integrals, tile_rows, destinations, source_terms, occ_energy, virt_energy):
    ny, nx, nz = (lax.axis_size(a) for a in GRP)
    nblk = lax.axis_size("xh") * lax.axis_size("k")
    groups = ny * nx * nz
    own = lax.axis_index(GRP).astype(jnp.int32)
    blk = lax.axis_index(BLK).astype(jnp.int32)
    x_lo = lax.axis_index("xl").astype(jnp.int32)
    owned, rows, full_width = amplitudes.shape
    all_tiles, dest = destinations.shape
    width = full_width // nblk
    sub = rows // nx
    slots = all_tiles * dest // groups
    columns, listed, _, size = integrals.shape

    x = cut_call(amplitudes, nx, nblk)
    x = lax.all_to_all(x, LINE, 0, 0, tiled=True)
    facts = [virt_energy.reshape(columns, size), tile_rows.astype(F32)]
    facts.append(jnp.zeros((columns, size - listed), F32))
    facts = jnp.concatenate(facts, axis=1)
    facts_across = swap(facts, 2, nblk)
    across = swap(integrals, 2, nblk)
    x = x.reshape(nx, nblk, sub, owned, width).transpose(1, 2, 0, 3, 4)
    x = lax.all_to_all(x.reshape(ny * nz, nx * owned, width), PLANE, 0, 0, tiled=True)
    table = x.reshape(all_tiles, width)

    dest_t = destinations.reshape(ny, nx, nz, owned, dest).transpose(4, 0, 2, 1, 3)
    slot_of, early, mine = rank_call(own.reshape(1), dest_t.reshape(dest, all_tiles), groups)
    outgoing = route_call(slot_of, early, table, slots)
    holders = [
        [g * nblk + quarter_of(g // nz % nx, q) for g in range(groups)] for q in range(nblk)
    ]
    outgoing = outgoing.reshape(groups, slots, width)
    incoming = lax.all_to_all(
        outgoing, GRP + BLK, 0, 0, axis_index_groups=holders, tiled=True
    )

    beside = swap(integrals, 1, nblk)
    pair = jnp.concatenate([facts, facts_across], axis=0)
    other = swap(pair, 1, nblk)
    facts = jnp.concatenate([facts, other[:columns], facts_across, other[columns:]], axis=0)
    named_tiles = facts[:, size : size + listed].astype(jnp.int32)
    y_of = named_tiles // (nx * nz * owned)
    x_of = (named_tiles // (nz * owned)) % nx
    z_of = (named_tiles // owned) % nz
    at = ((y_of * nz + z_of) * nx + x_of) * owned + named_tiles % owned
    where = jnp.arange(all_tiles, dtype=jnp.int32)
    slot = jnp.max(jnp.where(at[:, :, None] == where, mine.reshape(1, 1, all_tiles), -1), axis=2)
    slot = slot.reshape(-1)
    diagonal = swap(across, 1, nblk)

    turned = turn_call(incoming, nblk, ny, nx, nz)

    def quarter(flip):
        return lax.dynamic_slice_in_dim(source_terms, quarter_of(x_lo, blk ^ flip) * width, width, 1)

    source_far = swap(quarter(2), 2, nblk)
    source_near = swap(quarter(1), 1, nblk)
    source_diagonal = swap(quarter(3), 3, nblk)

    occ = occ_energy.reshape(1, full_width)
    virt = facts[:, :size]
    mine = jnp.stack([blk, quarter_of(x_lo, blk)])
    local = ladder_call(
        slot, mine, 0, (integrals, beside), turned, (quarter(0), source_near), occ, virt
    )
    done = ladder_call(
        slot,
        mine,
        2,
        (across, diagonal),
        turned,
        (source_far, source_diagonal),
        occ,
        virt,
        ready=local,
        places=(0, 1, 2, 3),
    )
    done = lax.all_to_all(done, BLK, 0, 0, tiled=True)
    parts = []
    for q in range(nblk):
        usual, other = done[q], done[quarter_of(1, q)]
        parts.append(usual if quarter_of(1, q) == q else jnp.where(x_lo == 1, other, usual))
    return jnp.concatenate(parts, axis=1)


def solution(mesh):
    n_grp = mesh.shape["grp"]
    fine = Mesh(mesh.devices.reshape(8, 2, n_grp // 16, 2, 2), GRP + BLK)
    every = GRP + BLK
    in_specs = (
        P(GRP, BLK, None),
        P(every, None, None, None),
        P(every, None),
        P(),
        P(every, None),
        P(),
        P(every),
    )
    return jax.shard_map(
        per_device, mesh=fine, in_specs=in_specs, out_specs=P(every, None), check_vma=False
    )
```

```python
import jax
import jax.numpy as jnp
from jax import lax
from jax.experimental import pallas as pl
from jax.experimental.pallas import tpu as pltpu
from jax.sharding import Mesh, PartitionSpec as P


GRP = ("y", "xl", "z")
BLK = ("xh", "k")
LINE = ("xl", "xh", "k")
PLANE = ("y", "z")
BF = jnp.bfloat16
F32 = jnp.float32
PARAMS = pltpu.CompilerParams(vmem_limit_bytes=48 * 1024 * 1024)


def quarter_of(x_lo, b):
    return b ^ ((x_lo & b & 1) << 1)


def rank_call(own, dest, groups):
    named_by, tiles = dest.shape
    lanes = 128
    half = tiles // 2 // lanes

    def body(own_ref, dest_ref, slot_ref, early_ref, mine_ref):
        ids = lax.broadcasted_iota(jnp.int32, (groups, lanes), 0)
        before = lax.broadcasted_iota(jnp.int32, (lanes, lanes), 0)
        after = lax.broadcasted_iota(jnp.int32, (lanes, lanes), 1)
        tri = (before < after).astype(F32).astype(BF)
        carry = jnp.zeros((groups, 1), F32)
        for i in range(tiles // lanes):
            if i == half:
                early_ref[...] = jnp.broadcast_to(carry, (groups, lanes))
            named = dest_ref[0:1, pl.ds(i * lanes, lanes)] == ids
            for l in range(1, named_by):
                named = named | (dest_ref[l : l + 1, pl.ds(i * lanes, lanes)] == ids)
            ones = named.astype(F32)
            earlier = jnp.dot(ones.astype(BF), tri, preferred_element_type=F32) + carry
            slot_ref[:, pl.ds(i * lanes, lanes)] = jnp.where(named, earlier, -1.0)
            carry = carry + jnp.sum(ones, axis=1, keepdims=True)
        mine_ref[...] = slot_ref[pl.ds(own_ref[0], 1), :].astype(jnp.int32)

    return pl.pallas_call(
        body,
        grid_spec=pltpu.PrefetchScalarGridSpec(
            num_scalar_prefetch=1,
            grid=(1,),
            in_specs=[pl.BlockSpec(dest.shape, lambda i, s: (0, 0))],
            out_specs=[
                pl.BlockSpec((groups, tiles), lambda i, s: (0, 0)),
                pl.BlockSpec((groups, lanes), lambda i, s: (0, 0)),
                pl.BlockSpec((1, tiles), lambda i, s: (0, 0)),
            ],
        ),
        out_shape=[
            jax.ShapeDtypeStruct((groups, tiles), F32),
            jax.ShapeDtypeStruct((groups, lanes), F32),
            jax.ShapeDtypeStruct((1, tiles), jnp.int32),
        ],
        compiler_params=PARAMS,
        name="rank",
    )(own, dest)


def route_call(slot, early, table, slots):
    groups, tiles = slot.shape
    width = table.shape[1]
    half = tiles // 2
    step = 32
    deep = 16

    def body(slot_ref, early_ref, table_ref, out_ref):
        one = jnp.asarray(1, BF)
        zero = jnp.asarray(0, BF)
        place = lax.broadcasted_iota(jnp.int32, (deep, half), 0)
        places = [(place + deep * q).astype(F32).astype(BF) for q in range(slots // deep)]
        rows = slot_ref[...]
        parts = []
        for d in range(step):
            lo = jnp.broadcast_to(rows[d : d + 1, :half], (deep, half)).astype(BF)
            hi = jnp.broadcast_to(rows[d : d + 1, half:], (deep, half)).astype(BF)
            for at in places:
                parts.append(jnp.where((lo == at) | (hi == at), one, zero))
        pick = jnp.concatenate(parts, axis=0)
        both = jnp.concatenate([table_ref[:half, :], table_ref[half:, :]], axis=1)
        got = jnp.dot(pick, both, preferred_element_type=F32)
        j = lax.broadcasted_iota(jnp.int32, (slots, width), 0).astype(F32)
        for d in range(step):
            late = j >= early_ref[d : d + 1, :]
            g = got[d * slots : (d + 1) * slots]
            out_ref[d * slots : (d + 1) * slots, :] = jnp.where(late, g[:, width:], g[:, :width]).astype(BF)

    return pl.pallas_call(
        body,
        grid=(groups // step,),
        in_specs=[
            pl.BlockSpec((step, tiles), lambda i: (i, 0)),
            pl.BlockSpec((step, width), lambda i: (i, 0)),
            pl.BlockSpec((tiles, width), lambda i: (0, 0)),
        ],
        out_specs=pl.BlockSpec((step * slots, width), lambda i: (i, 0)),
        out_shape=jax.ShapeDtypeStruct((groups * slots, width), BF),
        compiler_params=PARAMS,
        name="route",
    )(slot, early, table)


def cut_call(amplitudes, nx, nblk):
    owned, rows, full_width = amplitudes.shape
    sub = rows // nx
    width = full_width // nblk

    def body(a_ref, out_ref):
        for h in range(nx):
            for q in range(nblk):
                part = a_ref[:, h * sub : (h + 1) * sub, q * width : (q + 1) * width]
                out_ref[h * nblk + quarter_of(h, q)] = jnp.swapaxes(part, 0, 1)

    return pl.pallas_call(
        body,
        grid=(1,),
        in_specs=[pl.BlockSpec(amplitudes.shape, lambda i: (0, 0, 0))],
        out_specs=pl.BlockSpec((nx * nblk, sub, owned, width), lambda i: (0, 0, 0, 0)),
        out_shape=jax.ShapeDtypeStruct((nx * nblk, sub, owned, width), BF),
        compiler_params=PARAMS,
        name="cut",
    )(amplitudes)


def turn_call(incoming, nblk, ny, nx, nz):
    depth, slots, width = incoming.shape
    step = 16
    low = ny // nblk

    def body(t_ref, out_ref):
        x = t_ref[...].reshape(nblk, low, nx, nz, step, width)
        order = [(b, y, h) for b in range(nblk) for h in range(nx) for y in range(low)]
        x = jnp.concatenate([x[b, y, h] for b, y, h in order], axis=0)
        x = jnp.swapaxes(x, 0, 1)
        for j in range(step):
            out_ref[j] = x[j].T

    return pl.pallas_call(
        body,
        grid=(slots // step,),
        in_specs=[pl.BlockSpec((depth, step, width), lambda i: (0, i, 0))],
        out_specs=pl.BlockSpec((step, width, depth), lambda i: (i, 0, 0)),
        out_shape=jax.ShapeDtypeStruct((slots, width, depth), BF),
        compiler_params=PARAMS,
        name="turn",
    )(incoming)


def ladder_call(slot, blk, flips, weights, turned, sources, occ, virt):
    columns, listed, depth, size = weights[0].shape
    width = turned.shape[1]
    owners = len(weights)
    some = 2

    def body(slot_ref, blk_ref, *refs):
        w_refs = refs[:owners]
        t_ref = refs[owners]
        s_refs = refs[owners + 1 : 2 * owners + 1]
        o_ref, v_ref, out_ref, held_ref, sems = refs[2 * owners + 1 :]
        for m in range(owners):
            for n in range(columns):
                at = m * columns + n
                pltpu.make_async_copy(w_refs[m].at[n], held_ref.at[at], sems.at[at]).start()
        for m in range(owners):
            to = blk_ref[0] ^ flips[m]

            def some_columns(i, _, m=m, to=to):
                for u in range(some):
                    n = i * some + u
                    at = m * columns + n
                    pltpu.make_async_copy(w_refs[m].at[n], held_ref.at[at], sems.at[at]).wait()
                    right, left = [], []
                    for r in range(listed):
                        s = slot_ref[at * listed + r]
                        w = held_ref[at, r]
                        hi = w.astype(BF)
                        lo = (w - hi.astype(F32)).astype(BF)
                        right.append(jnp.concatenate([hi, lo], axis=1))
                        t = t_ref[jnp.maximum(s, 0)]
                        left.append(jnp.where(s >= 0, t, jnp.zeros_like(t)))
                    right = jnp.concatenate(right, axis=0)
                    left = jnp.concatenate(left, axis=1)
                    acc = jnp.dot(left, right, preferred_element_type=F32)
                    part = (acc[:, :size] + acc[:, size:]).T
                    rows = pl.ds(n * size, size)
                    total = s_refs[m][rows, :].astype(F32) + part
                    v = jnp.broadcast_to(v_ref[pl.ds(at, 1), :], (size, size)).T
                    out_ref[to, rows, :] = (total / (v + o_ref[...])).astype(BF)
                return 0

            lax.fori_loop(0, columns // some, some_columns, 0)

    def whole(x):
        return pl.BlockSpec(x.shape, lambda i, s, b: (0,) * x.ndim)

    return pl.pallas_call(
        body,
        grid_spec=pltpu.PrefetchScalarGridSpec(
            num_scalar_prefetch=2,
            grid=(1,),
            in_specs=[pl.BlockSpec(memory_space=pl.ANY)] * owners
            + [whole(turned)]
            + [whole(x) for x in sources]
            + [pl.BlockSpec((1, width), lambda i, s, b: (0, b[1])), whole(virt)],
            out_specs=pl.BlockSpec((owners, columns * size, width), lambda i, s, b: (0, 0, 0)),
            scratch_shapes=[
                pltpu.VMEM((owners * columns, listed, depth, size), F32),
                pltpu.SemaphoreType.DMA((owners * columns,)),
            ],
        ),
        out_shape=jax.ShapeDtypeStruct((owners, columns * size, width), BF),
        compiler_params=pltpu.CompilerParams(vmem_limit_bytes=48 * 1024 * 1024),
        name="ladder",
    )(slot, blk, *weights, turned, *sources, occ, virt)


def swap(x, flip, n):
    return lax.ppermute(x, BLK, [(b, b ^ flip) for b in range(n)])


def per_device(amplitudes, integrals, tile_rows, destinations, source_terms, occ_energy, virt_energy):
    ny, nx, nz = (lax.axis_size(a) for a in GRP)
    nblk = lax.axis_size("xh") * lax.axis_size("k")
    groups = ny * nx * nz
    own = lax.axis_index(GRP).astype(jnp.int32)
    blk = lax.axis_index(BLK).astype(jnp.int32)
    x_lo = lax.axis_index("xl").astype(jnp.int32)
    owned, rows, full_width = amplitudes.shape
    all_tiles, dest = destinations.shape
    width = full_width // nblk
    sub = rows // nx
    slots = all_tiles * dest // groups
    columns, listed, _, size = integrals.shape

    x = cut_call(amplitudes, nx, nblk)
    x = lax.all_to_all(x, LINE, 0, 0, tiled=True)
    facts = [virt_energy.reshape(columns, size), tile_rows.astype(F32)]
    facts.append(jnp.zeros((columns, size - listed), F32))
    facts = jnp.concatenate(facts, axis=1)
    facts_across = swap(facts, 2, nblk)
    across = swap(integrals, 2, nblk)
    x = x.reshape(nx, nblk, sub, owned, width).transpose(1, 2, 0, 3, 4)
    x = lax.all_to_all(x.reshape(ny * nz, nx * owned, width), PLANE, 0, 0, tiled=True)
    table = x.reshape(all_tiles, width)

    dest_t = destinations.reshape(ny, nx, nz, owned, dest).transpose(4, 0, 2, 1, 3)
    slot_of, early, mine = rank_call(own.reshape(1), dest_t.reshape(dest, all_tiles), groups)
    outgoing = route_call(slot_of, early, table, slots)
    holders = [
        [g * nblk + quarter_of(g // nz % nx, q) for g in range(groups)] for q in range(nblk)
    ]
    outgoing = outgoing.reshape(groups, slots, width)
    incoming = lax.all_to_all(
        outgoing, GRP + BLK, 0, 0, axis_index_groups=holders, tiled=True
    )

    beside = swap(integrals, 1, nblk)
    pair = jnp.concatenate([facts, facts_across], axis=0)
    other = swap(pair, 1, nblk)
    facts = jnp.concatenate([facts, other[:columns], facts_across, other[columns:]], axis=0)
    named_tiles = facts[:, size : size + listed].astype(jnp.int32)
    y_of = named_tiles // (nx * nz * owned)
    x_of = (named_tiles // (nz * owned)) % nx
    z_of = (named_tiles // owned) % nz
    at = ((y_of * nz + z_of) * nx + x_of) * owned + named_tiles % owned
    where = jnp.arange(all_tiles, dtype=jnp.int32)
    slot = jnp.max(jnp.where(at[:, :, None] == where, mine.reshape(1, 1, all_tiles), -1), axis=2)
    slot = slot.reshape(-1)
    diagonal = swap(across, 1, nblk)

    turned = turn_call(incoming, nblk, ny, nx, nz)

    def quarter(flip):
        return lax.dynamic_slice_in_dim(source_terms, quarter_of(x_lo, blk ^ flip) * width, width, 1)

    source_far = swap(quarter(2), 2, nblk)
    source_near = swap(quarter(1), 1, nblk)
    source_diagonal = swap(quarter(3), 3, nblk)

    occ = occ_energy.reshape(1, full_width)
    virt = facts[:, :size]
    mine = jnp.stack([blk, quarter_of(x_lo, blk)])
    done = ladder_call(
        slot,
        mine,
        (0, 1, 2, 3),
        (integrals, beside, across, diagonal),
        turned,
        (quarter(0), source_near, source_far, source_diagonal),
        occ,
        virt,
    )
    done = lax.all_to_all(done, BLK, 0, 0, tiled=True)
    x_lo, done = lax.optimization_barrier((x_lo, done))
    parts = []
    for q in range(nblk):
        usual, other = done[q], done[quarter_of(1, q)]
        parts.append(usual if quarter_of(1, q) == q else jnp.where(x_lo == 1, other, usual))
    return jnp.concatenate(parts, axis=1)


def solution(mesh):
    n_grp = mesh.shape["grp"]
    fine = Mesh(mesh.devices.reshape(8, 2, n_grp // 16, 2, 2), GRP + BLK)
    every = GRP + BLK
    in_specs = (
        P(GRP, BLK, None),
        P(every, None, None, None),
        P(every, None),
        P(),
        P(every, None),
        P(),
        P(every),
    )
    return jax.shard_map(
        per_device, mesh=fine, in_specs=in_specs, out_specs=P(every, None), check_vma=False
    )
```

```python
import jax
import jax.numpy as jnp
from jax import lax
from jax.experimental import pallas as pl
from jax.experimental.pallas import tpu as pltpu
from jax.sharding import Mesh, PartitionSpec as P


GRP = ("y", "xl", "z")
BLK = ("xh", "k")
LINE = ("xl", "xh", "k")
PLANE = ("y", "z")
BF = jnp.bfloat16
F32 = jnp.float32
PARAMS = pltpu.CompilerParams(vmem_limit_bytes=48 * 1024 * 1024)


def quarter_of(x_lo, b):
    return b ^ ((x_lo & b & 1) << 1)


def rank_call(own, dest, groups):
    named_by, tiles = dest.shape
    lanes = 128
    half = tiles // 2 // lanes

    def body(own_ref, dest_ref, slot_ref, early_ref, mine_ref):
        ids = lax.broadcasted_iota(jnp.int32, (groups, lanes), 0)
        before = lax.broadcasted_iota(jnp.int32, (lanes, lanes), 0)
        after = lax.broadcasted_iota(jnp.int32, (lanes, lanes), 1)
        tri = (before < after).astype(F32).astype(BF)
        carry = jnp.zeros((groups, 1), F32)
        for i in range(tiles // lanes):
            if i == half:
                early_ref[...] = jnp.broadcast_to(carry, (groups, lanes))
            named = dest_ref[0:1, pl.ds(i * lanes, lanes)] == ids
            for l in range(1, named_by):
                named = named | (dest_ref[l : l + 1, pl.ds(i * lanes, lanes)] == ids)
            ones = named.astype(F32)
            earlier = jnp.dot(ones.astype(BF), tri, preferred_element_type=F32) + carry
            slot_ref[:, pl.ds(i * lanes, lanes)] = jnp.where(named, earlier, -1.0)
            carry = carry + jnp.sum(ones, axis=1, keepdims=True)
        mine_ref[...] = slot_ref[pl.ds(own_ref[0], 1), :].astype(jnp.int32)

    return pl.pallas_call(
        body,
        grid_spec=pltpu.PrefetchScalarGridSpec(
            num_scalar_prefetch=1,
            grid=(1,),
            in_specs=[pl.BlockSpec(dest.shape, lambda i, s: (0, 0))],
            out_specs=[
                pl.BlockSpec((groups, tiles), lambda i, s: (0, 0)),
                pl.BlockSpec((groups, lanes), lambda i, s: (0, 0)),
                pl.BlockSpec((1, tiles), lambda i, s: (0, 0)),
            ],
        ),
        out_shape=[
            jax.ShapeDtypeStruct((groups, tiles), F32),
            jax.ShapeDtypeStruct((groups, lanes), F32),
            jax.ShapeDtypeStruct((1, tiles), jnp.int32),
        ],
        compiler_params=PARAMS,
        name="rank",
    )(own, dest)


def route_call(slot, early, table, slots):
    groups, tiles = slot.shape
    width = table.shape[1]
    half = tiles // 2
    step = 32
    deep = 16

    def body(slot_ref, early_ref, table_ref, out_ref):
        one = jnp.asarray(1, BF)
        zero = jnp.asarray(0, BF)
        place = lax.broadcasted_iota(jnp.int32, (deep, half), 0)
        places = [(place + deep * q).astype(F32).astype(BF) for q in range(slots // deep)]
        rows = slot_ref[...]
        parts = []
        for d in range(step):
            lo = jnp.broadcast_to(rows[d : d + 1, :half], (deep, half)).astype(BF)
            hi = jnp.broadcast_to(rows[d : d + 1, half:], (deep, half)).astype(BF)
            for at in places:
                parts.append(jnp.where((lo == at) | (hi == at), one, zero))
        pick = jnp.concatenate(parts, axis=0)
        both = jnp.concatenate([table_ref[:half, :], table_ref[half:, :]], axis=1)
        got = jnp.dot(pick, both, preferred_element_type=F32)
        j = lax.broadcasted_iota(jnp.int32, (slots, width), 0).astype(F32)
        for d in range(step):
            late = j >= early_ref[d : d + 1, :]
            g = got[d * slots : (d + 1) * slots]
            out_ref[d * slots : (d + 1) * slots, :] = jnp.where(late, g[:, width:], g[:, :width]).astype(BF)

    return pl.pallas_call(
        body,
        grid=(groups // step,),
        in_specs=[
            pl.BlockSpec((step, tiles), lambda i: (i, 0)),
            pl.BlockSpec((step, width), lambda i: (i, 0)),
            pl.BlockSpec((tiles, width), lambda i: (0, 0)),
        ],
        out_specs=pl.BlockSpec((step * slots, width), lambda i: (i, 0)),
        out_shape=jax.ShapeDtypeStruct((groups * slots, width), BF),
        compiler_params=PARAMS,
        name="route",
    )(slot, early, table)


def cut_call(amplitudes, nx, nblk):
    owned, rows, full_width = amplitudes.shape
    sub = rows // nx
    width = full_width // nblk

    def body(a_ref, out_ref):
        for h in range(nx):
            for q in range(nblk):
                part = a_ref[:, h * sub : (h + 1) * sub, q * width : (q + 1) * width]
                out_ref[h * nblk + quarter_of(h, q)] = jnp.swapaxes(part, 0, 1)

    return pl.pallas_call(
        body,
        grid=(1,),
        in_specs=[pl.BlockSpec(amplitudes.shape, lambda i: (0, 0, 0))],
        out_specs=pl.BlockSpec((nx * nblk, sub, owned, width), lambda i: (0, 0, 0, 0)),
        out_shape=jax.ShapeDtypeStruct((nx * nblk, sub, owned, width), BF),
        compiler_params=PARAMS,
        name="cut",
    )(amplitudes)


def turn_call(incoming, nblk, ny, nx, nz):
    depth, slots, width = incoming.shape
    step = 16
    low = ny // nblk

    def body(t_ref, out_ref):
        x = t_ref[...].reshape(nblk, low, nx, nz, step, width)
        order = [(b, y, h) for b in range(nblk) for h in range(nx) for y in range(low)]
        x = jnp.concatenate([x[b, y, h] for b, y, h in order], axis=0)
        x = jnp.swapaxes(x, 0, 1)
        for j in range(step):
            out_ref[j] = x[j].T

    return pl.pallas_call(
        body,
        grid=(slots // step,),
        in_specs=[pl.BlockSpec((depth, step, width), lambda i: (0, i, 0))],
        out_specs=pl.BlockSpec((step, width, depth), lambda i: (i, 0, 0)),
        out_shape=jax.ShapeDtypeStruct((slots, width, depth), BF),
        compiler_params=PARAMS,
        name="turn",
    )(incoming)


def ladder_call(slot, blk, flips, weights, turned, sources, occ, virt):
    columns, listed, depth, size = weights[0].shape
    width = turned.shape[1]
    owners = len(weights)
    some = 2

    def body(slot_ref, blk_ref, *refs):
        w_refs = refs[:owners]
        t_ref = refs[owners]
        s_refs = refs[owners + 1 : 2 * owners + 1]
        o_ref, v_ref = refs[2 * owners + 1 : 2 * owners + 3]
        out_refs = refs[2 * owners + 3 : 3 * owners + 3]
        held_ref, sems = refs[-2:]
        for m in range(owners):
            for n in range(columns):
                at = m * columns + n
                pltpu.make_async_copy(w_refs[m].at[n], held_ref.at[at], sems.at[at]).start()
        for m in range(owners):
            owner = flips[m]

            def some_columns(i, _, m=m, owner=owner):
                for u in range(some):
                    n = i * some + u
                    at = m * columns + n
                    pltpu.make_async_copy(w_refs[m].at[n], held_ref.at[at], sems.at[at]).wait()
                    named = owner * columns + n
                    right, left = [], []
                    for r in range(listed):
                        s = slot_ref[named * listed + r]
                        w = held_ref[at, r]
                        hi = w.astype(BF)
                        lo = (w - hi.astype(F32)).astype(BF)
                        right.append(jnp.concatenate([hi, lo], axis=1))
                        t = t_ref[jnp.maximum(s, 0)]
                        left.append(jnp.where(s >= 0, t, jnp.zeros_like(t)))
                    right = jnp.concatenate(right, axis=0)
                    left = jnp.concatenate(left, axis=1)
                    acc = jnp.dot(left, right, preferred_element_type=F32)
                    part = (acc[:, :size] + acc[:, size:]).T
                    rows = pl.ds(n * size, size)
                    total = s_refs[m][rows, :].astype(F32) + part
                    v = jnp.broadcast_to(v_ref[pl.ds(named, 1), :], (size, size)).T
                    out_refs[m][rows, :] = (total / (v + o_ref[...])).astype(BF)
                return 0

            lax.fori_loop(0, columns // some, some_columns, 0)

    def whole(x):
        return pl.BlockSpec(x.shape, lambda i, s, b: (0,) * x.ndim)

    return pl.pallas_call(
        body,
        grid_spec=pltpu.PrefetchScalarGridSpec(
            num_scalar_prefetch=2,
            grid=(1,),
            in_specs=[pl.BlockSpec(memory_space=pl.ANY)] * owners
            + [whole(turned)]
            + [whole(x) for x in sources]
            + [pl.BlockSpec((1, width), lambda i, s, b: (0, b[1])), whole(virt)],
            out_specs=[pl.BlockSpec((columns * size, width), lambda i, s, b: (0, 0))] * owners,
            scratch_shapes=[
                pltpu.VMEM((owners * columns, listed, depth, size), F32),
                pltpu.SemaphoreType.DMA((owners * columns,)),
            ],
        ),
        out_shape=[jax.ShapeDtypeStruct((columns * size, width), BF)] * owners,
        compiler_params=pltpu.CompilerParams(vmem_limit_bytes=48 * 1024 * 1024),
        name="ladder",
    )(slot, blk, *weights, turned, *sources, occ, virt)


def place_call(at, pieces):
    rows, width = pieces[0].shape
    count = len(pieces)

    def body(at_ref, *refs):
        for j in range(count):

            @pl.when(pl.program_id(0) == j)
            def _(j=j):
                refs[-1][...] = refs[j][...]

    return pl.pallas_call(
        body,
        grid_spec=pltpu.PrefetchScalarGridSpec(
            num_scalar_prefetch=1,
            grid=(count,),
            in_specs=[pl.BlockSpec((rows, width), lambda i, b: (0, 0))] * count,
            out_specs=pl.BlockSpec((rows, width), lambda i, b: (0, b[i])),
        ),
        out_shape=jax.ShapeDtypeStruct((rows, width * count), BF),
        compiler_params=PARAMS,
        name="place",
    )(at, *pieces)


def swap(x, flip, n):
    return lax.ppermute(x, BLK, [(b, b ^ flip) for b in range(n)])


def per_device(amplitudes, integrals, tile_rows, destinations, source_terms, occ_energy, virt_energy):
    ny, nx, nz = (lax.axis_size(a) for a in GRP)
    nblk = lax.axis_size("xh") * lax.axis_size("k")
    groups = ny * nx * nz
    own = lax.axis_index(GRP).astype(jnp.int32)
    blk = lax.axis_index(BLK).astype(jnp.int32)
    x_lo = lax.axis_index("xl").astype(jnp.int32)
    owned, rows, full_width = amplitudes.shape
    all_tiles, dest = destinations.shape
    width = full_width // nblk
    sub = rows // nx
    slots = all_tiles * dest // groups
    columns, listed, _, size = integrals.shape

    x = cut_call(amplitudes, nx, nblk)
    x = lax.all_to_all(x, LINE, 0, 0, tiled=True)
    facts = [virt_energy.reshape(columns, size), tile_rows.astype(F32)]
    facts.append(jnp.zeros((columns, size - listed), F32))
    facts = jnp.concatenate(facts, axis=1)
    facts_across = swap(facts, 2, nblk)
    across = swap(integrals, 2, nblk)
    x = x.reshape(nx, nblk, sub, owned, width).transpose(1, 2, 0, 3, 4)
    x = lax.all_to_all(x.reshape(ny * nz, nx * owned, width), PLANE, 0, 0, tiled=True)
    table = x.reshape(all_tiles, width)

    dest_t = destinations.reshape(ny, nx, nz, owned, dest).transpose(4, 0, 2, 1, 3)
    slot_of, early, mine = rank_call(own.reshape(1), dest_t.reshape(dest, all_tiles), groups)
    outgoing = route_call(slot_of, early, table, slots)
    holders = [
        [g * nblk + quarter_of(g // nz % nx, q) for g in range(groups)] for q in range(nblk)
    ]
    outgoing = outgoing.reshape(groups, slots, width)
    incoming = lax.all_to_all(
        outgoing, GRP + BLK, 0, 0, axis_index_groups=holders, tiled=True
    )

    beside = swap(integrals, 1, nblk)
    pair = jnp.concatenate([facts, facts_across], axis=0)
    other = swap(pair, 1, nblk)
    facts = jnp.concatenate([facts, other[:columns], facts_across, other[columns:]], axis=0)
    named_tiles = facts[:, size : size + listed].astype(jnp.int32)
    y_of = named_tiles // (nx * nz * owned)
    x_of = (named_tiles // (nz * owned)) % nx
    z_of = (named_tiles // owned) % nz
    at = ((y_of * nz + z_of) * nx + x_of) * owned + named_tiles % owned
    where = jnp.arange(all_tiles, dtype=jnp.int32)
    slot = jnp.max(jnp.where(at[:, :, None] == where, mine.reshape(1, 1, all_tiles), -1), axis=2)
    slot = slot.reshape(-1)
    diagonal = swap(across, 1, nblk)

    turned = turn_call(incoming, nblk, ny, nx, nz)

    def quarter(flip):
        return lax.dynamic_slice_in_dim(source_terms, quarter_of(x_lo, blk ^ flip) * width, width, 1)

    source_far = swap(quarter(2), 2, nblk)
    source_near = swap(quarter(1), 1, nblk)
    source_diagonal = swap(quarter(3), 3, nblk)

    occ = occ_energy.reshape(1, full_width)
    virt = facts[:, :size]
    mine = jnp.stack([blk, quarter_of(x_lo, blk)])
    one, two = ladder_call(
        slot, mine, (2, 3), (across, diagonal), turned, (source_far, source_diagonal), occ, virt
    )
    mine, one, two = lax.optimization_barrier((mine, one, two))
    far = swap(one, 2, nblk)
    farther = swap(two, 3, nblk)
    home, near = ladder_call(
        slot, mine, (0, 1), (integrals, beside), turned, (quarter(0), source_near), occ, virt
    )
    near = swap(near, 1, nblk)
    at = jnp.stack([quarter_of(x_lo, blk ^ flip) for flip in range(nblk)])
    return place_call(at, (home, near, far, farther))


def solution(mesh):
    n_grp = mesh.shape["grp"]
    fine = Mesh(mesh.devices.reshape(8, 2, n_grp // 16, 2, 2), GRP + BLK)
    every = GRP + BLK
    in_specs = (
        P(GRP, BLK, None),
        P(every, None, None, None),
        P(every, None),
        P(),
        P(every, None),
        P(),
        P(every),
    )
    return jax.shard_map(
        per_device, mesh=fine, in_specs=in_specs, out_specs=P(every, None), check_vma=False
    )
```

```python
import jax
import jax.numpy as jnp
from jax import lax
from jax.experimental import pallas as pl
from jax.experimental.pallas import tpu as pltpu
from jax.sharding import Mesh, PartitionSpec as P


GRP = ("y", "xl", "z")
BLK = ("xh", "k")
LINE = ("xl", "xh", "k")
PLANE = ("y", "z")
BF = jnp.bfloat16
F32 = jnp.float32
PARAMS = pltpu.CompilerParams(vmem_limit_bytes=48 * 1024 * 1024)


def quarter_of(x_lo, b):
    return b ^ ((x_lo & b & 1) << 1)


def rank_call(own, dest, groups):
    named_by, tiles = dest.shape
    lanes = 128
    half = tiles // 2 // lanes

    def body(own_ref, dest_ref, slot_ref, early_ref, mine_ref):
        ids = lax.broadcasted_iota(jnp.int32, (groups, lanes), 0)
        before = lax.broadcasted_iota(jnp.int32, (lanes, lanes), 0)
        after = lax.broadcasted_iota(jnp.int32, (lanes, lanes), 1)
        tri = (before < after).astype(F32).astype(BF)
        carry = jnp.zeros((groups, 1), F32)
        for i in range(tiles // lanes):
            if i == half:
                early_ref[...] = jnp.broadcast_to(carry, (groups, lanes))
            named = dest_ref[0:1, pl.ds(i * lanes, lanes)] == ids
            for l in range(1, named_by):
                named = named | (dest_ref[l : l + 1, pl.ds(i * lanes, lanes)] == ids)
            ones = named.astype(F32)
            earlier = jnp.dot(ones.astype(BF), tri, preferred_element_type=F32) + carry
            slot_ref[:, pl.ds(i * lanes, lanes)] = jnp.where(named, earlier, -1.0)
            carry = carry + jnp.sum(ones, axis=1, keepdims=True)
        mine_ref[...] = slot_ref[pl.ds(own_ref[0], 1), :].astype(jnp.int32)

    return pl.pallas_call(
        body,
        grid_spec=pltpu.PrefetchScalarGridSpec(
            num_scalar_prefetch=1,
            grid=(1,),
            in_specs=[pl.BlockSpec(dest.shape, lambda i, s: (0, 0))],
            out_specs=[
                pl.BlockSpec((groups, tiles), lambda i, s: (0, 0)),
                pl.BlockSpec((groups, lanes), lambda i, s: (0, 0)),
                pl.BlockSpec((1, tiles), lambda i, s: (0, 0)),
            ],
        ),
        out_shape=[
            jax.ShapeDtypeStruct((groups, tiles), F32),
            jax.ShapeDtypeStruct((groups, lanes), F32),
            jax.ShapeDtypeStruct((1, tiles), jnp.int32),
        ],
        compiler_params=PARAMS,
        name="rank",
    )(own, dest)


def route_call(slot, early, table, slots):
    groups, tiles = slot.shape
    width = table.shape[1]
    half = tiles // 2
    step = 32
    deep = 16

    def body(slot_ref, early_ref, table_ref, out_ref):
        one = jnp.asarray(1, BF)
        zero = jnp.asarray(0, BF)
        place = lax.broadcasted_iota(jnp.int32, (deep, half), 0)
        places = [(place + deep * q).astype(F32).astype(BF) for q in range(slots // deep)]
        rows = slot_ref[...]
        parts = []
        for d in range(step):
            lo = jnp.broadcast_to(rows[d : d + 1, :half], (deep, half)).astype(BF)
            hi = jnp.broadcast_to(rows[d : d + 1, half:], (deep, half)).astype(BF)
            for at in places:
                parts.append(jnp.where((lo == at) | (hi == at), one, zero))
        pick = jnp.concatenate(parts, axis=0)
        both = jnp.concatenate([table_ref[:half, :], table_ref[half:, :]], axis=1)
        got = jnp.dot(pick, both, preferred_element_type=F32)
        j = lax.broadcasted_iota(jnp.int32, (slots, width), 0).astype(F32)
        for d in range(step):
            late = j >= early_ref[d : d + 1, :]
            g = got[d * slots : (d + 1) * slots]
            out_ref[d * slots : (d + 1) * slots, :] = jnp.where(late, g[:, width:], g[:, :width]).astype(BF)

    return pl.pallas_call(
        body,
        grid=(groups // step,),
        in_specs=[
            pl.BlockSpec((step, tiles), lambda i: (i, 0)),
            pl.BlockSpec((step, width), lambda i: (i, 0)),
            pl.BlockSpec((tiles, width), lambda i: (0, 0)),
        ],
        out_specs=pl.BlockSpec((step * slots, width), lambda i: (i, 0)),
        out_shape=jax.ShapeDtypeStruct((groups * slots, width), BF),
        compiler_params=PARAMS,
        name="route",
    )(slot, early, table)


def cut_call(amplitudes, nx, nblk):
    owned, rows, full_width = amplitudes.shape
    sub = rows // nx
    width = full_width // nblk

    def body(a_ref, out_ref):
        for h in range(nx):
            for q in range(nblk):
                part = a_ref[:, h * sub : (h + 1) * sub, q * width : (q + 1) * width]
                out_ref[h * nblk + quarter_of(h, q)] = jnp.swapaxes(part, 0, 1)

    return pl.pallas_call(
        body,
        grid=(1,),
        in_specs=[pl.BlockSpec(amplitudes.shape, lambda i: (0, 0, 0))],
        out_specs=pl.BlockSpec((nx * nblk, sub, owned, width), lambda i: (0, 0, 0, 0)),
        out_shape=jax.ShapeDtypeStruct((nx * nblk, sub, owned, width), BF),
        compiler_params=PARAMS,
        name="cut",
    )(amplitudes)


def turn_call(incoming, nblk, ny, nx, nz):
    depth, slots, width = incoming.shape
    step = 16
    low = ny // nblk

    def body(t_ref, out_ref):
        x = t_ref[...].reshape(nblk, low, nx, nz, step, width)
        order = [(b, y, h) for b in range(nblk) for h in range(nx) for y in range(low)]
        x = jnp.concatenate([x[b, y, h] for b, y, h in order], axis=0)
        x = jnp.swapaxes(x, 0, 1)
        for j in range(step):
            out_ref[j] = x[j].T

    return pl.pallas_call(
        body,
        grid=(slots // step,),
        in_specs=[pl.BlockSpec((depth, step, width), lambda i: (0, i, 0))],
        out_specs=pl.BlockSpec((step, width, depth), lambda i: (i, 0, 0)),
        out_shape=jax.ShapeDtypeStruct((slots, width, depth), BF),
        compiler_params=PARAMS,
        name="turn",
    )(incoming)


def ladder_call(slot, blk, flips, weights, turned, sources, occ, virt):
    columns, listed, depth, size = weights[0].shape
    width = turned.shape[1]
    owners = len(weights)
    some = 2

    def body(slot_ref, blk_ref, *refs):
        w_refs = refs[:owners]
        t_ref = refs[owners]
        s_refs = refs[owners + 1 : 2 * owners + 1]
        o_ref, v_ref = refs[2 * owners + 1 : 2 * owners + 3]
        out_refs = refs[2 * owners + 3 : 3 * owners + 3]
        held_ref, sems = refs[-2:]
        for m in range(owners):
            for n in range(columns):
                at = m * columns + n
                pltpu.make_async_copy(w_refs[m].at[n], held_ref.at[at], sems.at[at]).start()
        for m in range(owners):
            owner = flips[m]

            def some_columns(i, _, m=m, owner=owner):
                for u in range(some):
                    n = i * some + u
                    at = m * columns + n
                    pltpu.make_async_copy(w_refs[m].at[n], held_ref.at[at], sems.at[at]).wait()
                    named = owner * columns + n
                    right, left = [], []
                    for r in range(listed):
                        s = slot_ref[named * listed + r]
                        w = held_ref[at, r]
                        hi = w.astype(BF)
                        lo = (w - hi.astype(F32)).astype(BF)
                        right.append(jnp.concatenate([hi, lo], axis=1))
                        t = t_ref[jnp.maximum(s, 0)]
                        left.append(jnp.where(s >= 0, t, jnp.zeros_like(t)))
                    right = jnp.concatenate(right, axis=0)
                    left = jnp.concatenate(left, axis=1)
                    acc = jnp.dot(left, right, preferred_element_type=F32)
                    part = (acc[:, :size] + acc[:, size:]).T
                    rows = pl.ds(n * size, size)
                    total = s_refs[m][rows, :].astype(F32) + part
                    v = jnp.broadcast_to(v_ref[pl.ds(named, 1), :], (size, size)).T
                    out_refs[m][rows, :] = (total / (v + o_ref[...])).astype(BF)
                return 0

            lax.fori_loop(0, columns // some, some_columns, 0)

    def whole(x):
        return pl.BlockSpec(x.shape, lambda i, s, b: (0,) * x.ndim)

    return pl.pallas_call(
        body,
        grid_spec=pltpu.PrefetchScalarGridSpec(
            num_scalar_prefetch=2,
            grid=(1,),
            in_specs=[pl.BlockSpec(memory_space=pl.ANY)] * owners
            + [whole(turned)]
            + [whole(x) for x in sources]
            + [pl.BlockSpec((1, width), lambda i, s, b: (0, b[1])), whole(virt)],
            out_specs=[pl.BlockSpec((columns * size, width), lambda i, s, b: (0, 0))] * owners,
            scratch_shapes=[
                pltpu.VMEM((owners * columns, listed, depth, size), F32),
                pltpu.SemaphoreType.DMA((owners * columns,)),
            ],
        ),
        out_shape=[jax.ShapeDtypeStruct((columns * size, width), BF)] * owners,
        compiler_params=pltpu.CompilerParams(vmem_limit_bytes=48 * 1024 * 1024),
        name="ladder",
    )(slot, blk, *weights, turned, *sources, occ, virt)


def swap(x, flip, n):
    return lax.ppermute(x, BLK, [(b, b ^ flip) for b in range(n)])


def per_device(amplitudes, integrals, tile_rows, destinations, source_terms, occ_energy, virt_energy):
    ny, nx, nz = (lax.axis_size(a) for a in GRP)
    nblk = lax.axis_size("xh") * lax.axis_size("k")
    groups = ny * nx * nz
    own = lax.axis_index(GRP).astype(jnp.int32)
    blk = lax.axis_index(BLK).astype(jnp.int32)
    x_lo = lax.axis_index("xl").astype(jnp.int32)
    owned, rows, full_width = amplitudes.shape
    all_tiles, dest = destinations.shape
    width = full_width // nblk
    sub = rows // nx
    slots = all_tiles * dest // groups
    columns, listed, _, size = integrals.shape

    x = cut_call(amplitudes, nx, nblk)
    x = lax.all_to_all(x, LINE, 0, 0, tiled=True)
    facts = [virt_energy.reshape(columns, size), tile_rows.astype(F32)]
    facts.append(jnp.zeros((columns, size - listed), F32))
    facts = jnp.concatenate(facts, axis=1)
    facts_across = swap(facts, 2, nblk)
    across = swap(integrals, 2, nblk)
    x = x.reshape(nx, nblk, sub, owned, width).transpose(1, 2, 0, 3, 4)
    x = lax.all_to_all(x.reshape(ny * nz, nx * owned, width), PLANE, 0, 0, tiled=True)
    table = x.reshape(all_tiles, width)

    dest_t = destinations.reshape(ny, nx, nz, owned, dest).transpose(4, 0, 2, 1, 3)
    slot_of, early, mine = rank_call(own.reshape(1), dest_t.reshape(dest, all_tiles), groups)
    outgoing = route_call(slot_of, early, table, slots)
    holders = [
        [g * nblk + quarter_of(g // nz % nx, q) for g in range(groups)] for q in range(nblk)
    ]
    outgoing = outgoing.reshape(groups, slots, width)
    incoming = lax.all_to_all(
        outgoing, GRP + BLK, 0, 0, axis_index_groups=holders, tiled=True
    )

    beside = swap(integrals, 1, nblk)
    pair = jnp.concatenate([facts, facts_across], axis=0)
    other = swap(pair, 1, nblk)
    facts = jnp.concatenate([facts, other[:columns], facts_across, other[columns:]], axis=0)
    named_tiles = facts[:, size : size + listed].astype(jnp.int32)
    y_of = named_tiles // (nx * nz * owned)
    x_of = (named_tiles // (nz * owned)) % nx
    z_of = (named_tiles // owned) % nz
    at = ((y_of * nz + z_of) * nx + x_of) * owned + named_tiles % owned
    where = jnp.arange(all_tiles, dtype=jnp.int32)
    slot = jnp.max(jnp.where(at[:, :, None] == where, mine.reshape(1, 1, all_tiles), -1), axis=2)
    slot = slot.reshape(-1)
    diagonal = swap(across, 1, nblk)

    turned = turn_call(incoming, nblk, ny, nx, nz)

    def quarter(flip):
        return lax.dynamic_slice_in_dim(source_terms, quarter_of(x_lo, blk ^ flip) * width, width, 1)

    source_far = swap(quarter(2), 2, nblk)
    source_near = swap(quarter(1), 1, nblk)
    source_diagonal = swap(quarter(3), 3, nblk)

    occ = occ_energy.reshape(1, full_width)
    virt = facts[:, :size]
    mine = jnp.stack([blk, quarter_of(x_lo, blk)])
    one, two = ladder_call(
        slot, mine, (2, 3), (across, diagonal), turned, (source_far, source_diagonal), occ, virt
    )
    mine, one, two = lax.optimization_barrier((mine, one, two))
    far = swap(one, 2, nblk)
    farther = swap(two, 3, nblk)
    home, near = ladder_call(
        slot, mine, (0, 1), (integrals, beside), turned, (quarter(0), source_near), occ, virt
    )
    near = swap(near, 1, nblk)
    parts = []
    for q in range(nblk):
        flip = blk ^ quarter_of(x_lo, q)
        low = jnp.where(flip == 0, home, near)
        high = jnp.where(flip == 2, far, farther)
        parts.append(jnp.where(flip < 2, low, high))
    return jnp.concatenate(parts, axis=1)


def solution(mesh):
    n_grp = mesh.shape["grp"]
    fine = Mesh(mesh.devices.reshape(8, 2, n_grp // 16, 2, 2), GRP + BLK)
    every = GRP + BLK
    in_specs = (
        P(GRP, BLK, None),
        P(every, None, None, None),
        P(every, None),
        P(),
        P(every, None),
        P(),
        P(every),
    )
    return jax.shard_map(
        per_device, mesh=fine, in_specs=in_specs, out_specs=P(every, None), check_vma=False
    )
```
